32 devices in a mesh: groups: 2 (over x), tm: 4 (over y, core), rows: 4 (over z).
Axes of the slice: x: 2, y: 2, z: 4, core: 2. Of those that a mesh axis runs over, the one named last changes fastest.
Arguments:
- features: bfloat16 [16, 8, 96, 512], P(('groups', 'tm'), 'rows'), parts along dimension 0, may hold values from -6 to 6
- spatial_weight: bfloat16 [3, 3, 512, 512], replicated, may hold values from -0.09375 to 0.09375
- temporal_weight: bfloat16 [3, 512, 512], replicated, may hold values from -0.15625 to 0.15625
- head_weight: bfloat16 [512, 16], replicated, may hold values from -0.25 to 0.25
- embed_weight: bfloat16 [64, 5120], replicated, may hold values from -0.75 to 0.75
- ada_scale: bfloat16 [5120], replicated, may hold values from -0.5 to 0.5
- ada_shift: bfloat16 [5120], replicated, may hold values from -3 to 3
- qkv_weight: bfloat16 [5120, 9216], P('tm', 'rows'), may hold values from -0.078125 to 0.078125
Outputs:
- qkv: float32 [3072, 9216], P(('groups', 'tm'), 'rows'), parts along dimension 0
The draws below stay inside these ranges and needn't reach their ends.
There are 2 independent parts, one for each index of `groups`. The reference program is written for one: setup_inputs(seed, part) draws one part's arguments, and reference() takes and returns one part's arrays. A program takes and returns all parts, laid end to end along the dimension named above; an argument that names none is the same for every part. Nothing has to cross between parts.
All inputs are finite; a program needn't handle non-finite values.
Results may differ from the reference program's by a relative error of at most 0.0056.
Values may be sent and summed in bfloat16 or wider, within the bound.
A program may use at most 128 MiB of HBM per device.

```python
import jax
import jax.numpy as jnp
from jax import lax

D = 5120
LATENT = 16
PATCH = 2
CH = 512
WIDTH = 96
FRAMES = 8
HEIGHT = 8
QKV = 9216
PDIM = 64
TOKENS = 1536


def block_levels(stream_key, dims, split, least, largest):
    def one(dim, shards_of):
        heights = jax.random.uniform(jax.random.fold_in(jax.random.fold_in(stream_key, 6), dim), (shards_of,), jnp.float32, least / len(split), largest / len(split))
        return jnp.repeat(jnp.exp(heights), dims[dim] // shards_of).reshape((-1,) + (1,) * (len(dims) - dim - 1))

    level = one(*split[0])
    for cut in split[1:]:
        level = level * one(*cut)
    return level


def scatter_about(own_key, dims, scale, limit, shards=(), held_as=jnp.bfloat16):
    values = scale * jax.random.normal(own_key, dims, jnp.float32)
    if shards:
        values = values * block_levels(own_key, dims, shards, -0.22, 0.18)
    return jnp.clip(values, -limit, limit).astype(held_as)


def setup_inputs(seed: int = 0, part: int = 0) -> dict:
    arg_keys = jax.random.split(jax.random.key(seed), 9)
    part_splits = jax.random.split(jax.random.fold_in(arg_keys[8], part), 9)
    return {
        "features": scatter_about(part_splits[0], (FRAMES, HEIGHT, WIDTH, CH), 1.0, 6.0, ((0, 4), (1, 4))),
        "spatial_weight": scatter_about(arg_keys[1], (3, 3, CH, CH), (9 * CH) ** -0.5, 0.09375),
        "temporal_weight": scatter_about(arg_keys[2], (3, CH, CH), (3 * CH) ** -0.5, 0.15625),
        "head_weight": scatter_about(arg_keys[3], (CH, LATENT), CH ** -0.5, 0.25),
        "embed_weight": scatter_about(arg_keys[4], (PDIM, D), PDIM ** -0.5, 0.75),
        "ada_scale": jnp.clip(jax.random.uniform(arg_keys[5], (D,), jnp.float32, -0.5, 0.5), -0.5, 0.5).astype(jnp.bfloat16),
        "ada_shift": scatter_about(arg_keys[6], (D,), 0.5, 3.0),
        "qkv_weight": scatter_about(arg_keys[7], (D, QKV), D ** -0.5, 0.078125, ((0, 4), (1, 4))),
    }


def norm_silu(values):
    scaled = values * jax.lax.rsqrt(lax.optimization_barrier(jnp.mean(values * values, axis=-1, keepdims=True)) + 1e-06)
    return jax.nn.silu(scaled)

def reference(features, spatial_weight, temporal_weight, head_weight, embed_weight, ada_scale, ada_shift, qkv_weight):
    activated = norm_silu(features.astype(jnp.float32)).astype(jnp.bfloat16)
    padded = jnp.pad(activated, ((0, 0), (1, 1), (1, 1), (0, 0)))
    spatial = jnp.zeros((FRAMES * HEIGHT * WIDTH, CH), jnp.float32)
    for tap_row in range(3):
        for tap_col in range(3):
            window = padded[:, tap_row:tap_row + HEIGHT, tap_col:tap_col + WIDTH].reshape(-1, CH)
            spatial = spatial + jnp.dot(window, spatial_weight[tap_row, tap_col], preferred_element_type=jnp.float32)
    mixed_act = norm_silu(spatial).astype(jnp.bfloat16).reshape(FRAMES, HEIGHT, WIDTH, CH)
    stacked = jnp.pad(mixed_act, ((2, 0), (0, 0), (0, 0), (0, 0)))
    temporal = jnp.zeros((FRAMES * HEIGHT * WIDTH, CH), jnp.float32)
    for tap in range(3):
        temporal = temporal + jnp.dot(stacked[tap:tap + FRAMES].reshape(-1, CH), temporal_weight[tap], preferred_element_type=jnp.float32)
    summed = features.astype(jnp.float32).reshape(-1, CH) + temporal
    latent = jnp.dot(norm_silu(summed).astype(jnp.bfloat16), head_weight, preferred_element_type=jnp.float32).astype(jnp.bfloat16)
    latent = latent.reshape(FRAMES, HEIGHT // PATCH, PATCH, WIDTH // PATCH, PATCH, LATENT)
    patches = jnp.transpose(latent, (0, 1, 3, 2, 4, 5)).reshape(TOKENS, PDIM)
    embedded = jnp.dot(patches, embed_weight, preferred_element_type=jnp.float32).astype(jnp.bfloat16)
    widened = lax.optimization_barrier(embedded).astype(jnp.float32)
    centered = widened - lax.optimization_barrier(jnp.mean(widened, axis=-1, keepdims=True))
    spread = lax.optimization_barrier(jnp.mean(centered * centered, axis=-1, keepdims=True))
    modulated = centered * lax.rsqrt(spread + 1e-06) * (1.0 + ada_scale.astype(jnp.float32)) + ada_shift.astype(jnp.float32)
    normalized = modulated.astype(jnp.bfloat16)
    return jnp.dot(normalized, qkv_weight, preferred_element_type=jnp.float32)
```

```python
import functools

import jax
import jax.numpy as jnp
from jax import lax
from jax.experimental import pallas as pl
from jax.experimental.pallas import tpu as pltpu
from jax.sharding import PartitionSpec as P

MESH = pl.DeviceIdType.MESH
PATCH = 2
LANES = 128
EPS = 1e-06
F32 = jnp.float32
BF16 = jnp.bfloat16


def dot(a, b):
    return jnp.dot(a, b, preferred_element_type=F32)


def dot_t(a, b):
    return lax.dot_general(a, b, (((1,), (1,)), ((), ())), preferred_element_type=F32)


def norm_silu(values):
    scaled = values * lax.rsqrt(jnp.mean(values * values, axis=-1, keepdims=True) + EPS)
    half = 0.5 * scaled
    return half + half * jnp.tanh(half)


def encode(
    n_groups, n_tm, n_rows, split, aligned,
    features, spatial_hbm, temporal_hbm, head_hbm, embed_hbm, part_ref, scale_ref, shift_ref, qkv_hbm,
    block_out, fold_out, shift_out, gram_out,
    feat, halo, taps, spat_w, temp_w, head_w, embed, wide, qkv_w, mixed, before, partial, lat,
    part_b, core_in, keep, cross, fold, shifts, shifts_in, gathered,
    load_sem, halo_send, halo_recv, mix_send, mix_recv, all_send, all_recv,
    fold_send, fold_recv, shift_send, shift_recv,
):
    group, tile, row = lax.axis_index("groups"), lax.axis_index("tm"), lax.axis_index("rows")
    frames, rows, columns, channels = features.shape
    depth, width = qkv_w.shape
    pdim = embed.shape[0]
    wide_all = embed.shape[1]
    blocks, block_rows = fold.shape[0], fold.shape[1]
    core = lax.rem(tile, 2)
    partners = [{"tm": tile + 1 - 2 * core}]
    if split:
        partners.append({"groups": 1 - group})
    step = 2
    while step < n_tm:
        partners.append({"tm": tile + step * (1 - 2 * lax.rem(tile // step, 2))})
        step *= 2
    reach = partners + [{"tm": lax.rem(tile + 1, n_tm)}, {"tm": lax.rem(tile + n_tm - 1, n_tm)}]
    reach += [{"rows": lax.rem(row + d, n_rows)} for d in range(1, n_rows)]

    barrier = pltpu.get_barrier_semaphore()
    for device in reach:
        pl.semaphore_signal(barrier, inc=1, device_id=device, device_id_type=MESH)

    def load(source, target, index):
        copy = pltpu.make_async_copy(source, target, load_sem.at[index])
        copy.start()
        return copy

    load_feat = load(features, feat, 0)
    load_spat = load(spatial_hbm, spat_w, 1)
    load_embed = load(embed_hbm, embed, 2)
    first = group * depth if split else 0
    load_qkv = load(qkv_hbm.at[pl.ds(pl.multiple_of(first, 16), depth)], qkv_w, 3)
    load_temp = load(temporal_hbm, temp_w, 4)
    load_head = load(head_hbm, head_w, 5)

    def remote(source, target, send, recv, device):
        return pltpu.make_async_remote_copy(
            src_ref=source, dst_ref=target, send_sem=send, recv_sem=recv,
            device_id=device, device_id_type=MESH,
        )

    up = remote(features.at[:, 0], halo.at[1], halo_send.at[0], halo_recv.at[1], {"rows": row - 1})
    down = remote(
        features.at[:, rows - 1], halo.at[0], halo_send.at[1], halo_recv.at[0], {"rows": row + 1}
    )
    has_above, has_below = row > 0, row < n_rows - 1
    has_before, has_after = tile > 0, tile < n_tm - 1

    pl.semaphore_wait(barrier, len(reach))

    @pl.when(has_above)
    def _():
        up.start()

    @pl.when(has_below)
    def _():
        down.start()

    @pl.when(jnp.logical_not(has_above))
    def _():
        halo[0] = jnp.zeros(halo.shape[1:], BF16)

    @pl.when(jnp.logical_not(has_below))
    def _():
        halo[1] = jnp.zeros(halo.shape[1:], BF16)

    @pl.when(jnp.logical_not(has_before))
    def _():
        before[...] = jnp.zeros(before.shape, BF16)

    span = 3 * channels
    column = lax.broadcasted_iota(jnp.int32, (columns, channels), 0)

    def spread_taps(values, place, frame):
        active = norm_silu(values.astype(F32))
        left = jnp.where(column == 0, 0.0, pltpu.roll(active, 1, 0))
        right = jnp.where(column == columns - 1, 0.0, pltpu.roll(active, columns - 1, 0))
        for k, shifted in enumerate((left, active, right)):
            taps[pl.ds(frame * columns, columns), pl.ds(place * span + k * channels, channels)] = (
                shifted.astype(BF16)
            )

    load_feat.wait()
    for frame in range(frames):
        for r in range(rows):
            spread_taps(feat[frame, r], r + 1, frame)
    load_spat.wait()
    inner = taps[:, span : 3 * span]
    partial[0] = dot(inner, spat_w[span : 3 * span])
    partial[1] = dot(inner, spat_w[0 : 2 * span])

    load_embed.wait()
    embedding = embed[...].astype(F32)
    mean = jnp.mean(embedding, axis=1, keepdims=True)
    if aligned:
        start = pl.multiple_of(tile * (wide_all // n_tm) + first, LANES)
        own = embed[:, pl.ds(start, depth)].astype(F32)
        scale = scale_ref[:, pl.ds(start, depth)].astype(F32)
        shift = shift_ref[:, pl.ds(start, depth)].astype(F32)
    else:
        own = part_ref[...].astype(F32)
        scale = scale_ref[...].astype(F32)
        shift = shift_ref[...].astype(F32)
    scaled = ((own - mean) * (1.0 + scale)).astype(BF16)
    rows16 = lax.broadcasted_iota(jnp.int32, (16, depth), 0)
    shift16 = jnp.where(rows16 == 0, jnp.broadcast_to(shift, (16, depth)), 0.0).astype(BF16)
    lhs = jnp.concatenate([scaled, shift16], axis=0)
    load_qkv.wait()
    chunk = width // 3
    for n in range(3):
        cols = pl.ds(n * chunk, chunk)
        terms = dot(lhs, qkv_w[:, cols])
        shifts[0, :, cols] = terms[pdim : pdim + 1]
        for b in range(blocks):
            piece = terms[b * block_rows : (b + 1) * block_rows]
            keep[b, :, cols] = piece
            part_b[b, :, cols] = piece.astype(BF16)

    half = blocks // 2
    mine = core * half + (group if split else 0)
    core_copy = remote(
        part_b.at[pl.ds((1 - core) * half, half)], core_in, fold_send.at[0], fold_recv.at[0], partners[0]
    )
    shift_copies = [
        remote(shifts.at[k], shifts_in.at[k], shift_send.at[k], shift_recv.at[k], device)
        for k, device in enumerate(partners)
    ]
    core_copy.start()
    shift_copies[0].start()

    def finish_row(r, frame_rows):
        for frame in range(frames):
            spread_taps(frame_rows[frame], 0 if r == 0 else rows + 1, frame)
        if r == 0:
            total = partial[0] + dot(taps[:, 0:span], spat_w[0:span])
        else:
            total = partial[1] + dot(taps[:, 3 * span :], spat_w[2 * span :])
        active = norm_silu(total).astype(BF16)
        for frame in range(frames):
            mixed[pl.ds(r * columns, columns), pl.ds(frame * channels, channels)] = active[
                frame * columns : (frame + 1) * columns
            ]
        copy = remote(
            mixed.at[pl.ds(r * columns, columns)], before.at[pl.ds(r * columns, columns)],
            mix_send.at[r], mix_recv.at[r], {"tm": tile + 1},
        )

        @pl.when(has_after)
        def _():
            copy.start()

        return copy

    @pl.when(has_above)
    def _():
        down.wait_recv()

    mix_copies = [finish_row(0, halo.at[0])]

    core_copy.wait()
    shift_copies[0].wait()
    cross_copies = []

    def summed(b, stage_in):
        return keep[b] + stage_in.astype(F32)

    if split:
        cross[0] = summed(core * half + 1 - group, core_in[1 - group]).astype(BF16)
        keep[mine] = summed(mine, core_in[group])
        x_in = 1
    else:
        keep[mine] = summed(mine, core_in[0])
        x_in = 0
    shifts[1] = shifts[0] + shifts_in[0]
    k = 1
    slot = 0

    def start_stage(k, slot):
        copy = remote(
            cross.at[2 * slot], cross.at[2 * slot + 1], fold_send.at[k], fold_recv.at[k], partners[k]
        )
        copy.start()
        shift_copies[k].start()
        return copy

    if not split:
        cross[0] = keep[mine].astype(BF16)
    stage = start_stage(k, slot)

    @pl.when(has_below)
    def _():
        up.wait_recv()

    mix_copies.append(finish_row(1, halo.at[1]))

    while k < len(partners):
        stage.wait()
        shift_copies[k].wait()
        keep[mine] = summed(mine, cross[2 * slot + 1])
        shifts[k + 1] = shifts[k] + shifts_in[k]
        k += 1
        slot += 1
        if k < len(partners):
            cross[2 * slot] = keep[mine].astype(BF16)
            stage = start_stage(k, slot)
    fold[mine] = keep[mine].astype(BF16)
    if split:
        share = remote(fold.at[mine], fold.at[mine], fold_send.at[k], fold_recv.at[k], partners[1])
        share.start()
        k += 1

    centred = embed[...].astype(F32) - mean
    high = centred.astype(BF16)
    wide[0:pdim] = high
    wide[pdim:] = (centred - high.astype(F32)).astype(BF16)
    products = dot_t(wide[...], wide[...])
    gram = (
        products[:pdim, :pdim] + products[:pdim, pdim:]
        + products[pdim:, :pdim] + products[pdim:, pdim:]
    ) * (1.0 / wide_all)
    for i in range(3):
        piece = gram.astype(BF16)
        gram_out[i] = piece
        gram = gram - piece.astype(F32)

    load_head.wait()
    lane = lax.broadcasted_iota(jnp.int32, (LANES, head_w.shape[0]), 0)
    latent_lane = lax.broadcasted_iota(jnp.int32, (LANES, head_w.shape[0]), 1)
    pair = PATCH * head_w.shape[0]
    heads = []
    for a in range(PATCH):
        pick = (lane >= a * pair) & (lane < (a + 1) * pair)
        pick = pick & (lax.rem(lane, head_w.shape[0]) == latent_lane)
        heads.append(dot(jnp.where(pick, 1.0, 0.0).astype(BF16), head_w[...]).astype(BF16))

    load_temp.wait()
    partial[0] = dot(mixed[:, :channels], temp_w[2 * channels :])
    partial[1] = dot(mixed[...], temp_w[channels:])

    if split:
        share.wait()
    widen = remote(
        fold.at[pl.ds(core * half, half)], fold.at[pl.ds(core * half, half)],
        fold_send.at[k], fold_recv.at[k], partners[0],
    )
    widen.start()

    @pl.when(has_before)
    def _():
        for copy in mix_copies:
            copy.wait_recv()

    for frame in range(frames):
        if frame == 0:
            total = partial[0] + dot(before[...], temp_w[: 2 * channels])
        else:
            total = partial[1] + dot(before[:, channels:], temp_w[:channels])
        total = total + jnp.concatenate([feat[frame, r].astype(F32) for r in range(rows)], axis=0)
        active = norm_silu(total).astype(BF16)
        lat[pl.ds(frame * columns, columns)] = dot_t(active[:columns], heads[0]) + dot_t(
            active[columns:], heads[1]
        )
    tokens = columns // PATCH
    out_lane = lax.broadcasted_iota(jnp.int32, (tokens, LANES), 1)
    even_lane = lax.rem(out_lane // head_w.shape[0], PATCH) == 0
    for frame in range(frames):
        even = lat[pl.ds(frame * columns, tokens, stride=PATCH), :]
        odd = lat[pl.ds(frame * columns + 1, tokens, stride=PATCH), :]
        gathered[row, frame] = jnp.where(even_lane, even, odd).astype(BF16)
    sends = [
        remote(
            gathered.at[row], gathered.at[row], all_send.at[d], all_recv.at[d],
            {"rows": lax.rem(row + d, n_rows)},
        )
        for d in range(1, n_rows)
    ]
    for copy in sends:
        copy.start()
    widen.wait()
    fold_out[...] = fold[...]
    shift_out[...] = shifts[len(partners)]
    for copy in sends:
        copy.wait()
    for p in range(n_rows):
        for frame in range(frames):
            block_out[frame, p] = gathered[p, frame]

    @pl.when(has_above)
    def _():
        up.wait_send()

    @pl.when(has_below)
    def _():
        down.wait_send()

    @pl.when(has_after)
    def _():
        for copy in mix_copies:
            copy.wait_send()


def project(pieces, block, fold, shift, gram, out, held, sems):
    pdim = fold.shape[0]
    tokens = block[:, :pdim]
    moved = dot(tokens, gram[0]) + dot(tokens, gram[1]) + dot(tokens, gram[2])
    spread = jnp.maximum(jnp.sum(moved * tokens.astype(F32), axis=-1, keepdims=True), 0.0)
    inverse = lax.rsqrt(spread + EPS)
    chunk = fold.shape[1] // pieces
    copies = []
    for n in range(pieces):
        cols = pl.ds(n * chunk, chunk)
        held[:, cols] = dot(tokens, fold[:, cols]) * inverse + shift[:, cols]
        copy = pltpu.make_async_copy(held.at[:, cols], out.at[:, cols], sems.at[n])
        copy.start()
        copies.append(copy)
    for copy in copies:
        copy.wait()


def per_device(
    n_groups, n_tm, n_rows,
    features, spatial_weight, temporal_weight, head_weight, embed_weight, ada_scale, ada_shift, qkv_weight,
):
    frames, rows, columns, channels = features.shape
    depth, width = qkv_weight.shape
    pdim, wide_all = embed_weight.shape
    latent = head_weight.shape[1]
    split = n_groups == 2
    depth = depth // 2 if split else depth
    aligned = depth % LANES == 0
    stages = n_tm.bit_length() - 1 + int(split)
    blocks = 4 if split else 2
    block_rows = pdim // blocks
    scale, shift, part = ada_scale[None], ada_shift[None], embed_weight
    if not aligned:
        start = lax.axis_index("tm") * qkv_weight.shape[0]
        if split:
            start = start + lax.axis_index("groups") * depth
        scale, shift, part = (lax.dynamic_slice_in_dim(v, start, depth, axis=1) for v in (scale, shift, part))
    hbm = pl.BlockSpec(memory_space=pl.ANY)
    vmem = pl.BlockSpec(memory_space=pltpu.VMEM)
    tokens = columns // PATCH
    dma = pltpu.SemaphoreType.DMA
    block, fold, shift_row, gram = pl.pallas_call(
        functools.partial(encode, n_groups, n_tm, n_rows, split, aligned),
        out_shape=(
            jax.ShapeDtypeStruct((frames, n_rows, tokens, LANES), BF16),
            jax.ShapeDtypeStruct((blocks, block_rows, width), BF16),
            jax.ShapeDtypeStruct((1, width), F32),
            jax.ShapeDtypeStruct((3, pdim, pdim), BF16),
        ),
        in_specs=[hbm, hbm, hbm, hbm, hbm, hbm if aligned else vmem, vmem, vmem, hbm],
        out_specs=(vmem, vmem, vmem, vmem),
        scratch_shapes=[
            pltpu.VMEM(features.shape, BF16),
            pltpu.VMEM((2, frames, columns, channels), BF16),
            pltpu.VMEM((frames * columns, (rows + 2) * 3 * channels), BF16),
            pltpu.VMEM((9 * channels, channels), BF16),
            pltpu.VMEM((3 * channels, channels), BF16),
            pltpu.VMEM((latent, channels), BF16),
            pltpu.VMEM((pdim, wide_all), BF16),
            pltpu.VMEM((2 * pdim, wide_all), BF16),
            pltpu.VMEM((depth, width), BF16),
            pltpu.VMEM((rows * columns, frames * channels), BF16),
            pltpu.VMEM((rows * columns, frames * channels), BF16),
            pltpu.VMEM((2, frames * columns, channels), F32),
            pltpu.VMEM((frames * columns, LANES), F32),
            pltpu.VMEM((blocks, block_rows, width), BF16),
            pltpu.VMEM((blocks // 2, block_rows, width), BF16),
            pltpu.VMEM((blocks, block_rows, width), F32),
            pltpu.VMEM((2 * (stages - 1), block_rows, width), BF16),
            pltpu.VMEM((blocks, block_rows, width), BF16),
            pltpu.VMEM((stages + 1, 1, width), F32),
            pltpu.VMEM((stages, 1, width), F32),
            pltpu.VMEM((n_rows, frames, tokens, LANES), BF16),
            dma((6,)),
            dma((2,)), dma((2,)),
            dma((rows,)), dma((rows,)),
            dma((n_rows,)), dma((n_rows,)),
            dma((stages + 2,)), dma((stages + 2,)),
            dma((stages,)), dma((stages,)),
        ],
        compiler_params=pltpu.CompilerParams(
            collective_id=0, has_side_effects=True, vmem_limit_bytes=56 * 2**20
        ),
        name="encode",
    )(
        features,
        spatial_weight.reshape(9 * channels, channels),
        temporal_weight.reshape(3 * channels, channels),
        head_weight.T,
        embed_weight,
        part,
        scale,
        shift,
        qkv_weight,
    )
    count = frames * n_rows * tokens
    pieces = 3
    return pl.pallas_call(
        functools.partial(project, pieces),
        out_shape=jax.ShapeDtypeStruct((count, width), F32),
        in_specs=[vmem] * 4,
        out_specs=hbm,
        scratch_shapes=[pltpu.VMEM((count, width), F32), dma((pieces,))],
        compiler_params=pltpu.CompilerParams(vmem_limit_bytes=32 * 2**20),
        name="project",
    )(block.reshape(count, LANES), fold.reshape(pdim, width), shift_row, gram)


def solution(mesh):
    return jax.shard_map(
        functools.partial(per_device, mesh.shape["groups"], mesh.shape["tm"], mesh.shape["rows"]),
        mesh=mesh,
        in_specs=(
            P(("groups", "tm"), "rows", None, None),
            P(),
            P(),
            P(),
            P(),
            P(),
            P(),
            P("tm", "rows"),
        ),
        out_specs=P(("groups", "tm"), "rows"),
        check_vma=False,
    )
```

```python
import functools

import jax
import jax.numpy as jnp
from jax import lax
from jax.experimental import pallas as pl
from jax.experimental.pallas import tpu as pltpu
from jax.sharding import PartitionSpec as P

MESH = pl.DeviceIdType.MESH
PATCH = 2
LANES = 128
EPS = 1e-06
F32 = jnp.float32
BF16 = jnp.bfloat16


def dot(a, b):
    return jnp.dot(a, b, preferred_element_type=F32)


def dot_t(a, b):
    return lax.dot_general(a, b, (((1,), (1,)), ((), ())), preferred_element_type=F32)


def norm_silu(values):
    scaled = values * lax.rsqrt(jnp.mean(values * values, axis=-1, keepdims=True) + EPS)
    half = 0.5 * scaled
    return half + half * jnp.tanh(half)


def encode(
    n_groups, n_tm, n_rows, split, aligned,
    features, spatial_hbm, temporal_hbm, head_hbm, embed_hbm, part_ref, scale_ref, shift_ref, qkv_hbm,
    block_out, fold_out, shift_out, gram_out,
    feat, halo, taps, spat_w, temp_w, head_w, embed, wide, qkv_w, mixed, before, partial, lat,
    part_b, core_in, keep, cross, fold, shifts, shifts_in, gathered, vectors,
    load_sem, halo_send, halo_recv, mix_send, mix_recv, all_send, all_recv,
    fold_send, fold_recv, shift_send, shift_recv,
):
    group, tile, row = lax.axis_index("groups"), lax.axis_index("tm"), lax.axis_index("rows")
    frames, rows, columns, channels = features.shape
    depth, width = qkv_w.shape
    pdim = embed.shape[0]
    wide_all = embed.shape[1]
    blocks, block_rows = fold.shape[0], fold.shape[1]
    core = lax.rem(tile, 2)
    partners = [{"tm": tile + 1 - 2 * core}]
    if split:
        partners.append({"groups": 1 - group})
    step = 2
    while step < n_tm:
        partners.append({"tm": tile + step * (1 - 2 * lax.rem(tile // step, 2))})
        step *= 2
    reach = partners + [{"tm": lax.rem(tile + 1, n_tm)}, {"tm": lax.rem(tile + n_tm - 1, n_tm)}]
    reach += [{"rows": lax.rem(row + d, n_rows)} for d in range(1, n_rows)]

    barrier = pltpu.get_barrier_semaphore()
    for device in reach:
        pl.semaphore_signal(barrier, inc=1, device_id=device, device_id_type=MESH)

    def load(source, target, index):
        copy = pltpu.make_async_copy(source, target, load_sem.at[index])
        copy.start()
        return copy

    load_feat = load(features, feat, 0)
    load_spat = load(spatial_hbm, spat_w, 1)
    load_embed = load(embed_hbm, embed, 2)
    first = group * depth if split else 0
    load_qkv = load(qkv_hbm.at[pl.ds(pl.multiple_of(first, 16), depth)], qkv_w, 3)
    load_temp = load(temporal_hbm, temp_w, 4)
    load_head = load(head_hbm, head_w, 5)

    def remote(source, target, send, recv, device):
        return pltpu.make_async_remote_copy(
            src_ref=source, dst_ref=target, send_sem=send, recv_sem=recv,
            device_id=device, device_id_type=MESH,
        )

    up = remote(features.at[:, 0], halo.at[1], halo_send.at[0], halo_recv.at[1], {"rows": row - 1})
    down = remote(
        features.at[:, rows - 1], halo.at[0], halo_send.at[1], halo_recv.at[0], {"rows": row + 1}
    )
    has_above, has_below = row > 0, row < n_rows - 1
    has_before, has_after = tile > 0, tile < n_tm - 1

    pl.semaphore_wait(barrier, len(reach))

    @pl.when(has_above)
    def _():
        up.start()

    @pl.when(has_below)
    def _():
        down.start()

    @pl.when(jnp.logical_not(has_above))
    def _():
        halo[0] = jnp.zeros(halo.shape[1:], BF16)

    @pl.when(jnp.logical_not(has_below))
    def _():
        halo[1] = jnp.zeros(halo.shape[1:], BF16)

    @pl.when(jnp.logical_not(has_before))
    def _():
        before[...] = jnp.zeros(before.shape, BF16)

    span = 3 * channels
    column = lax.broadcasted_iota(jnp.int32, (columns, channels), 0)

    def spread_taps(values, place, frame):
        active = norm_silu(values.astype(F32))
        left = jnp.where(column == 0, 0.0, pltpu.roll(active, 1, 0))
        right = jnp.where(column == columns - 1, 0.0, pltpu.roll(active, columns - 1, 0))
        for k, shifted in enumerate((left, active, right)):
            taps[pl.ds(frame * columns, columns), pl.ds(place * span + k * channels, channels)] = (
                shifted.astype(BF16)
            )

    load_feat.wait()
    for frame in range(frames):
        for r in range(rows):
            spread_taps(feat[frame, r], r + 1, frame)
    load_spat.wait()
    inner = taps[:, span : 3 * span]
    partial[0] = dot(inner, spat_w[span : 3 * span])
    partial[1] = dot(inner, spat_w[0 : 2 * span])

    load_embed.wait()
    embedding = embed[...].astype(F32)
    mean = jnp.mean(embedding, axis=1, keepdims=True)
    if aligned:
        start = pl.multiple_of(tile * (wide_all // n_tm) + first, LANES)
        own = embed[:, pl.ds(start, depth)].astype(F32)
        vectors[0] = scale_ref[...].astype(F32)
        vectors[1] = shift_ref[...].astype(F32)
        at = start // LANES
        scale, shift = (
            jnp.concatenate([vectors[v, pl.ds(at + j, 1)] for j in range(depth // LANES)], axis=1)
            for v in range(2)
        )
    else:
        own = part_ref[...].astype(F32)
        scale = scale_ref[...].astype(F32)
        shift = shift_ref[...].astype(F32)
    scaled = ((own - mean) * (1.0 + scale)).astype(BF16)
    rows16 = lax.broadcasted_iota(jnp.int32, (16, depth), 0)
    shift16 = jnp.where(rows16 == 0, jnp.broadcast_to(shift, (16, depth)), 0.0).astype(BF16)
    lhs = jnp.concatenate([scaled, shift16], axis=0)
    load_qkv.wait()
    chunk = width // 3
    for n in range(3):
        cols = pl.ds(n * chunk, chunk)
        terms = dot(lhs, qkv_w[:, cols])
        shifts[0, :, cols] = terms[pdim : pdim + 1]
        for b in range(blocks):
            piece = terms[b * block_rows : (b + 1) * block_rows]
            keep[b, :, cols] = piece
            part_b[b, :, cols] = piece.astype(BF16)

    half = blocks // 2
    mine = core * half + (group if split else 0)
    core_copy = remote(
        part_b.at[pl.ds((1 - core) * half, half)], core_in, fold_send.at[0], fold_recv.at[0], partners[0]
    )
    shift_copies = [
        remote(shifts.at[k], shifts_in.at[k], shift_send.at[k], shift_recv.at[k], device)
        for k, device in enumerate(partners)
    ]
    core_copy.start()
    shift_copies[0].start()

    def finish_row(r, frame_rows):
        for frame in range(frames):
            spread_taps(frame_rows[frame], 0 if r == 0 else rows + 1, frame)
        if r == 0:
            total = partial[0] + dot(taps[:, 0:span], spat_w[0:span])
        else:
            total = partial[1] + dot(taps[:, 3 * span :], spat_w[2 * span :])
        active = norm_silu(total).astype(BF16)
        for frame in range(frames):
            mixed[pl.ds(r * columns, columns), pl.ds(frame * channels, channels)] = active[
                frame * columns : (frame + 1) * columns
            ]
        copy = remote(
            mixed.at[pl.ds(r * columns, columns)], before.at[pl.ds(r * columns, columns)],
            mix_send.at[r], mix_recv.at[r], {"tm": tile + 1},
        )

        @pl.when(has_after)
        def _():
            copy.start()

        return copy

    @pl.when(has_above)
    def _():
        down.wait_recv()

    mix_copies = [finish_row(0, halo.at[0])]

    core_copy.wait()
    shift_copies[0].wait()
    cross_copies = []

    def summed(b, stage_in):
        return keep[b] + stage_in.astype(F32)

    if split:
        cross[0] = summed(core * half + 1 - group, core_in[1 - group]).astype(BF16)
        keep[mine] = summed(mine, core_in[group])
        x_in = 1
    else:
        keep[mine] = summed(mine, core_in[0])
        x_in = 0
    shifts[1] = shifts[0] + shifts_in[0]
    k = 1
    slot = 0

    def start_stage(k, slot):
        copy = remote(
            cross.at[2 * slot], cross.at[2 * slot + 1], fold_send.at[k], fold_recv.at[k], partners[k]
        )
        copy.start()
        shift_copies[k].start()
        return copy

    if not split:
        cross[0] = keep[mine].astype(BF16)
    stage = start_stage(k, slot)

    @pl.when(has_below)
    def _():
        up.wait_recv()

    mix_copies.append(finish_row(1, halo.at[1]))

    while k < len(partners):
        stage.wait()
        shift_copies[k].wait()
        keep[mine] = summed(mine, cross[2 * slot + 1])
        shifts[k + 1] = shifts[k] + shifts_in[k]
        k += 1
        slot += 1
        if k < len(partners):
            cross[2 * slot] = keep[mine].astype(BF16)
            stage = start_stage(k, slot)
    fold[mine] = keep[mine].astype(BF16)
    if split:
        share = remote(fold.at[mine], fold.at[mine], fold_send.at[k], fold_recv.at[k], partners[1])
        share.start()
        k += 1

    centred = embed[...].astype(F32) - mean
    high = centred.astype(BF16)
    wide[0:pdim] = high
    wide[pdim:] = (centred - high.astype(F32)).astype(BF16)
    products = dot_t(wide[...], wide[...])
    gram = (
        products[:pdim, :pdim] + products[:pdim, pdim:]
        + products[pdim:, :pdim] + products[pdim:, pdim:]
    ) * (1.0 / wide_all)
    for i in range(3):
        piece = gram.astype(BF16)
        gram_out[i] = piece
        gram = gram - piece.astype(F32)

    load_head.wait()
    lane = lax.broadcasted_iota(jnp.int32, (LANES, head_w.shape[0]), 0)
    latent_lane = lax.broadcasted_iota(jnp.int32, (LANES, head_w.shape[0]), 1)
    pair = PATCH * head_w.shape[0]
    heads = []
    for a in range(PATCH):
        pick = (lane >= a * pair) & (lane < (a + 1) * pair)
        pick = pick & (lax.rem(lane, head_w.shape[0]) == latent_lane)
        heads.append(dot(jnp.where(pick, 1.0, 0.0).astype(BF16), head_w[...]).astype(BF16))

    load_temp.wait()
    partial[0] = dot(mixed[:, :channels], temp_w[2 * channels :])
    partial[1] = dot(mixed[...], temp_w[channels:])

    if split:
        share.wait()
    widen = remote(
        fold.at[pl.ds(core * half, half)], fold.at[pl.ds(core * half, half)],
        fold_send.at[k], fold_recv.at[k], partners[0],
    )
    widen.start()

    @pl.when(has_before)
    def _():
        for copy in mix_copies:
            copy.wait_recv()

    for frame in range(frames):
        if frame == 0:
            total = partial[0] + dot(before[...], temp_w[: 2 * channels])
        else:
            total = partial[1] + dot(before[:, channels:], temp_w[:channels])
        total = total + jnp.concatenate([feat[frame, r].astype(F32) for r in range(rows)], axis=0)
        active = norm_silu(total).astype(BF16)
        lat[pl.ds(frame * columns, columns)] = dot_t(active[:columns], heads[0]) + dot_t(
            active[columns:], heads[1]
        )
    tokens = columns // PATCH
    out_lane = lax.broadcasted_iota(jnp.int32, (tokens, LANES), 1)
    even_lane = lax.rem(out_lane // head_w.shape[0], PATCH) == 0
    for frame in range(frames):
        even = lat[pl.ds(frame * columns, tokens, stride=PATCH), :]
        odd = lat[pl.ds(frame * columns + 1, tokens, stride=PATCH), :]
        gathered[row, frame] = jnp.where(even_lane, even, odd).astype(BF16)
    sends = [
        remote(
            gathered.at[row], gathered.at[row], all_send.at[d], all_recv.at[d],
            {"rows": lax.rem(row + d, n_rows)},
        )
        for d in range(1, n_rows)
    ]
    for copy in sends:
        copy.start()
    widen.wait()
    fold_out[...] = fold[...]
    shift_out[...] = shifts[len(partners)]
    for copy in sends:
        copy.wait()
    for p in range(n_rows):
        for frame in range(frames):
            block_out[frame, p] = gathered[p, frame]

    @pl.when(has_above)
    def _():
        up.wait_send()

    @pl.when(has_below)
    def _():
        down.wait_send()

    @pl.when(has_after)
    def _():
        for copy in mix_copies:
            copy.wait_send()


def project(pieces, block, fold, shift, gram, out, held, sems):
    pdim = fold.shape[0]
    tokens = block[:, :pdim]
    moved = dot(tokens, gram[0]) + dot(tokens, gram[1]) + dot(tokens, gram[2])
    spread = jnp.maximum(jnp.sum(moved * tokens.astype(F32), axis=-1, keepdims=True), 0.0)
    inverse = lax.rsqrt(spread + EPS)
    chunk = fold.shape[1] // pieces
    copies = []
    for n in range(pieces):
        cols = pl.ds(n * chunk, chunk)
        held[:, cols] = dot(tokens, fold[:, cols]) * inverse + shift[:, cols]
        copy = pltpu.make_async_copy(held.at[:, cols], out.at[:, cols], sems.at[n])
        copy.start()
        copies.append(copy)
    for copy in copies:
        copy.wait()


def per_device(
    n_groups, n_tm, n_rows,
    features, spatial_weight, temporal_weight, head_weight, embed_weight, ada_scale, ada_shift, qkv_weight,
):
    frames, rows, columns, channels = features.shape
    depth, width = qkv_weight.shape
    pdim, wide_all = embed_weight.shape
    latent = head_weight.shape[1]
    split = n_groups == 2
    depth = depth // 2 if split else depth
    aligned = depth % LANES == 0
    stages = n_tm.bit_length() - 1 + int(split)
    blocks = 4 if split else 2
    block_rows = pdim // blocks
    part = embed_weight
    scale, shift = (v.reshape(wide_all // LANES, LANES) for v in (ada_scale, ada_shift))
    if not aligned:
        scale, shift = ada_scale[None], ada_shift[None]
        start = lax.axis_index("tm") * qkv_weight.shape[0]
        if split:
            start = start + lax.axis_index("groups") * depth
        scale, shift, part = (lax.dynamic_slice_in_dim(v, start, depth, axis=1) for v in (scale, shift, part))
    hbm = pl.BlockSpec(memory_space=pl.ANY)
    vmem = pl.BlockSpec(memory_space=pltpu.VMEM)
    tokens = columns // PATCH
    dma = pltpu.SemaphoreType.DMA
    block, fold, shift_row, gram = pl.pallas_call(
        functools.partial(encode, n_groups, n_tm, n_rows, split, aligned),
        out_shape=(
            pltpu.VMEM((frames, n_rows, tokens, LANES), BF16),
            pltpu.VMEM((blocks, block_rows, width), BF16),
            pltpu.VMEM((1, width), F32),
            pltpu.VMEM((3, pdim, pdim), BF16),
        ),
        in_specs=[hbm, hbm, hbm, hbm, hbm, hbm if aligned else vmem, vmem, vmem, hbm],
        out_specs=(vmem, vmem, vmem, vmem),
        scratch_shapes=[
            pltpu.VMEM(features.shape, BF16),
            pltpu.VMEM((2, frames, columns, channels), BF16),
            pltpu.VMEM((frames * columns, (rows + 2) * 3 * channels), BF16),
            pltpu.VMEM((9 * channels, channels), BF16),
            pltpu.VMEM((3 * channels, channels), BF16),
            pltpu.VMEM((latent, channels), BF16),
            pltpu.VMEM((pdim, wide_all), BF16),
            pltpu.VMEM((2 * pdim, wide_all), BF16),
            pltpu.VMEM((depth, width), BF16),
            pltpu.VMEM((rows * columns, frames * channels), BF16),
            pltpu.VMEM((rows * columns, frames * channels), BF16),
            pltpu.VMEM((2, frames * columns, channels), F32),
            pltpu.VMEM((frames * columns, LANES), F32),
            pltpu.VMEM((blocks, block_rows, width), BF16),
            pltpu.VMEM((blocks // 2, block_rows, width), BF16),
            pltpu.VMEM((blocks, block_rows, width), F32),
            pltpu.VMEM((2 * (stages - 1), block_rows, width), BF16),
            pltpu.VMEM((blocks, block_rows, width), BF16),
            pltpu.VMEM((stages + 1, 1, width), F32),
            pltpu.VMEM((stages, 1, width), F32),
            pltpu.VMEM((n_rows, frames, tokens, LANES), BF16),
            pltpu.VMEM((2, wide_all // LANES, LANES), F32),
            dma((6,)),
            dma((2,)), dma((2,)),
            dma((rows,)), dma((rows,)),
            dma((n_rows,)), dma((n_rows,)),
            dma((stages + 2,)), dma((stages + 2,)),
            dma((stages,)), dma((stages,)),
        ],
        compiler_params=pltpu.CompilerParams(
            collective_id=0, has_side_effects=True, vmem_limit_bytes=56 * 2**20
        ),
        name="encode",
    )(
        features,
        spatial_weight.reshape(9 * channels, channels),
        temporal_weight.reshape(3 * channels, channels),
        head_weight.T,
        embed_weight,
        part,
        scale,
        shift,
        qkv_weight,
    )
    count = frames * n_rows * tokens
    pieces = 3
    return pl.pallas_call(
        functools.partial(project, pieces),
        out_shape=jax.ShapeDtypeStruct((count, width), F32),
        in_specs=[vmem] * 4,
        out_specs=hbm,
        scratch_shapes=[pltpu.VMEM((count, width), F32), dma((pieces,))],
        compiler_params=pltpu.CompilerParams(vmem_limit_bytes=32 * 2**20),
        name="project",
    )(block.reshape(count, LANES), fold.reshape(pdim, width), shift_row, gram)


def solution(mesh):
    return jax.shard_map(
        functools.partial(per_device, mesh.shape["groups"], mesh.shape["tm"], mesh.shape["rows"]),
        mesh=mesh,
        in_specs=(
            P(("groups", "tm"), "rows", None, None),
            P(),
            P(),
            P(),
            P(),
            P(),
            P(),
            P("tm", "rows"),
        ),
        out_specs=P(("groups", "tm"), "rows"),
        check_vma=False,
    )
```

```python
import functools

import jax
import jax.numpy as jnp
from jax import lax
from jax.experimental import pallas as pl
from jax.experimental.pallas import tpu as pltpu
from jax.sharding import PartitionSpec as P

MESH = pl.DeviceIdType.MESH
PATCH = 2
LANES = 128
EPS = 1e-06
F32 = jnp.float32
BF16 = jnp.bfloat16


def dot(a, b):
    return jnp.dot(a, b, preferred_element_type=F32)


def dot_t(a, b):
    return lax.dot_general(a, b, (((1,), (1,)), ((), ())), preferred_element_type=F32)


def norm_silu(values):
    scaled = values * lax.rsqrt(jnp.mean(values * values, axis=-1, keepdims=True) + EPS)
    half = 0.5 * scaled
    return half + half * jnp.tanh(half)


def encode(
    n_tm, n_rows, split, aligned,
    features, spatial_hbm, temporal_hbm, head_hbm, embed_hbm, part_hbm, scale_hbm, shift_hbm, qkv_hbm,
    block_out, fold_out, shift_out, gram_out,
    feat, halo, taps, spat_w, temp_w, head_w, embed, part, scale_v, shift_v, vectors, wide, qkv_w,
    mixed, before, partial, lat, part_b, core_in, keep, cross, quad_in, stage, fold, shifts, shifts_in, gathered, heads,
    load_sem, halo_send, halo_recv, mix_send, mix_recv, all_send, all_recv,
    fold_send, fold_recv, shift_send, shift_recv, relay,
):
    group, tile, row = lax.axis_index("groups"), lax.axis_index("tm"), lax.axis_index("rows")
    frames, rows, columns, channels = features.shape
    depth, width = qkv_w.shape
    pdim, wide_all = embed.shape
    latent = head_w.shape[0]
    _, quads, block_rows, _ = fold.shape
    has_above, has_below = row > 0, row < n_rows - 1
    has_before, has_after = tile > 0, tile < n_tm - 1
    near = [({"rows": row - 1}, has_above), ({"rows": row + 1}, has_below)]
    count_rows = has_above.astype(jnp.int32) + has_below.astype(jnp.int32)
    count_tiles = has_before.astype(jnp.int32) + has_after.astype(jnp.int32)
    core = lax.rem(tile, 2)
    other_core = {"tm": tile + 1 - 2 * core}

    def flipped(bit):
        return tile + bit * (1 - 2 * lax.rem(tile // bit, 2))

    bits = [("tm", lax.rem(tile // 2, 2), flipped(2))] if n_tm >= 4 else []
    if split:
        bits.append(("groups", group, 1 - group))
    mine = sum((bit[1] * 2**n for n, bit in enumerate(bits)), 0)
    direct = []
    for mask in range(1, quads):
        chosen = [n for n in range(len(bits)) if mask >> n & 1]
        place = mine + sum(2**n * (1 - 2 * bits[n][1]) for n in chosen)
        direct.append(({bits[n][0]: bits[n][2] for n in chosen}, place))
    later = []
    step = 4
    while step < n_tm:
        later.append({"tm": flipped(step)})
        step *= 2
    partners = [other_core] + [device for device, _ in direct] + later

    def signal(sem, device):
        pl.semaphore_signal(sem, inc=1, device_id=device, device_id_type=MESH)

    barrier = pltpu.get_barrier_semaphore()
    for device in partners:
        signal(barrier, device)
    for device, there in near + [({"tm": tile - 1}, has_before), ({"tm": tile + 1}, has_after)]:

        @pl.when(there)
        def _():
            signal(barrier, device)

    def load(source, target, index):
        copy = pltpu.make_async_copy(source, target, load_sem.at[index])
        copy.start()
        return copy

    first = group * depth if split else 0
    load_feat = load(features, feat, 0)
    load_embed = load(embed_hbm, embed, 1)
    load_scale = load(scale_hbm, scale_v, 2)
    load_shift = load(shift_hbm, shift_v, 3)
    if not aligned:
        load_part = load(part_hbm, part, 4)
    load_qkv = load(qkv_hbm.at[pl.ds(pl.multiple_of(first, 16), depth)], qkv_w, 5)
    load_spat = load(spatial_hbm, spat_w, 6)
    load_temp = load(temporal_hbm, temp_w, 7)
    load_head = load(head_hbm, head_w, 8)

    def remote(source, target, send, recv, device):
        return pltpu.make_async_remote_copy(
            src_ref=source, dst_ref=target, send_sem=send, recv_sem=recv,
            device_id=device, device_id_type=MESH,
        )

    ups, downs = [], []
    for f in range(frames):
        ups.append(
            remote(features.at[f, 0], halo.at[f, 1], halo_send.at[f, 0], halo_recv.at[f, 1], near[0][0])
        )
        downs.append(
            remote(
                features.at[f, rows - 1], halo.at[f, 0], halo_send.at[f, 1], halo_recv.at[f, 0], near[1][0]
            )
        )

    pl.semaphore_wait(barrier, len(partners) + count_rows + count_tiles)
    for f in range(frames):

        @pl.when(has_above)
        def _():
            ups[f].start()

        @pl.when(has_below)
        def _():
            downs[f].start()

    phases = max(n_rows - 2, 0)
    done_phases = [0]

    def tell(phase):
        if phase < phases:
            for device, there in near:

                @pl.when(there)
                def _():
                    signal(relay.at[phase], device)

    def next_phase():
        phase = done_phases[0]
        if phase < phases:
            pl.semaphore_wait(relay.at[phase], count_rows)
            tell(phase + 1)
            done_phases[0] = phase + 1

    tell(0)

    @pl.when(jnp.logical_not(has_above))
    def _():
        for f in range(frames):
            halo[f, 0] = jnp.zeros(halo.shape[2:], BF16)

    @pl.when(jnp.logical_not(has_below))
    def _():
        for f in range(frames):
            halo[f, 1] = jnp.zeros(halo.shape[2:], BF16)

    @pl.when(jnp.logical_not(has_before))
    def _():
        before[...] = jnp.zeros(before.shape, BF16)

    span = 3 * channels
    column = lax.broadcasted_iota(jnp.int32, (columns, channels), 0)

    def spread_taps(values, place, frame):
        active = norm_silu(values.astype(F32))
        left = jnp.where(column == 0, 0.0, pltpu.roll(active, 1, 0))
        right = jnp.where(column == columns - 1, 0.0, pltpu.roll(active, columns - 1, 0))
        for k, shifted in enumerate((left, active, right)):
            taps[pl.ds(frame * columns, columns), pl.ds(place * span + k * channels, channels)] = (
                shifted.astype(BF16)
            )

    load_embed.wait()
    load_scale.wait()
    load_shift.wait()
    mean = jnp.mean(embed[...].astype(F32), axis=1, keepdims=True)
    if aligned:
        start = pl.multiple_of(tile * (wide_all // n_tm) + first, LANES)
        own = embed[:, pl.ds(start, depth)].astype(F32)
        vectors[0] = scale_v[...].astype(F32)
        vectors[1] = shift_v[...].astype(F32)
        at = start // LANES
        scale, shift = (
            jnp.concatenate([vectors[v, pl.ds(at + j, 1)] for j in range(depth // LANES)], axis=1)
            for v in range(2)
        )
    else:
        load_part.wait()
        own, scale, shift = part[...].astype(F32), scale_v[...].astype(F32), shift_v[...].astype(F32)
    scaled = ((own - mean) * (1.0 + scale)).astype(BF16)
    rows16 = lax.broadcasted_iota(jnp.int32, (16, depth), 0)
    shift16 = jnp.where(rows16 == 0, jnp.broadcast_to(shift, (16, depth)), 0.0).astype(BF16)
    lhs = jnp.concatenate([scaled, shift16], axis=0)
    load_qkv.wait()
    chunk = width // 3
    for n in range(3):
        cols = pl.ds(n * chunk, chunk)
        terms = dot(lhs, qkv_w[:, cols])
        shifts[0, :, cols] = terms[pdim : pdim + 1]
        for side in range(2):
            for b in range(quads):
                low = (side * quads + b) * block_rows
                piece = terms[low : low + block_rows]
                keep[side, b, :, cols] = piece
                part_b[side, b, :, cols] = piece.astype(BF16)

    core_copies = [
        remote(part_b.at[1 - core], core_in, fold_send.at[0], fold_recv.at[0], other_core),
        remote(shifts.at[0], shifts_in.at[0], shift_send.at[0], shift_recv.at[0], other_core),
    ]
    for copy in core_copies:
        copy.start()

    load_feat.wait()
    for f in range(frames):
        for r in range(rows):
            spread_taps(feat[f, r], r + 1, f)
    load_spat.wait()
    inner = taps[:, span : 3 * span]
    direct_copies = []
    for r in range(rows):
        total = dot(inner, spat_w[(1 - r) * span : (3 - r) * span])
        for f in range(frames):
            partial[f, pl.ds(r * columns, columns)] = total[f * columns : (f + 1) * columns]
        if r == 0:
            for copy in core_copies:
                copy.wait()
            shifts[1] = shifts[0] + shifts_in[0]
            for b in range(quads):
                cross[b] = (keep[core, b] + core_in[b].astype(F32)).astype(BF16)
            for m, (device, place) in enumerate(direct, 1):
                direct_copies += [
                    remote(cross.at[place], quad_in.at[m], fold_send.at[m], fold_recv.at[m], device),
                    remote(shifts.at[1], shifts_in.at[m], shift_send.at[m], shift_recv.at[m], device),
                ]
            for copy in direct_copies:
                copy.start()
    next_phase()

    def finish_frame(f):
        @pl.when(has_above)
        def _():
            downs[f].wait_recv()

        @pl.when(has_below)
        def _():
            ups[f].wait_recv()

        spread_taps(halo[f, 0], 0, f)
        spread_taps(halo[f, 1], rows + 1, f)
        here = pl.ds(f * columns, columns)
        copies = []
        for r, (place, weights) in enumerate(
            ((0, spat_w[0:span]), (3 * span, spat_w[2 * span : 3 * span]))
        ):
            lines = pl.ds(r * columns, columns)
            total = partial[f, lines] + dot(taps[here, pl.ds(place, span)], weights)
            mixed[f, lines] = norm_silu(total).astype(BF16)
            copies.append(
                remote(
                    mixed.at[f, lines], before.at[f, lines], mix_send.at[f, r], mix_recv.at[f, r],
                    {"tm": tile + 1},
                )
            )

            @pl.when(has_after)
            def _():
                copies[-1].start()

        return copies

    mix_copies = finish_frame(0)
    next_phase()
    mix_copies += finish_frame(1)
    next_phase()

    load_head.wait()
    lane = lax.broadcasted_iota(jnp.int32, (latent, LANES), 1)
    latent_lane = lax.broadcasted_iota(jnp.int32, (latent, LANES), 0)
    pair = PATCH * latent
    for f in range(frames):
        for a in range(PATCH):
            low = f * pdim + a * pair
            pick = (lane >= low) & (lane < low + pair) & (lax.rem(lane, latent) == latent_lane)
            spread_head = lax.dot_general(
                head_w[...], jnp.where(pick, 1.0, 0.0).astype(BF16), (((0,), (0,)), ((), ())),
                preferred_element_type=F32,
            )
            heads[PATCH * f + a] = spread_head.astype(BF16)
    load_temp.wait()
    partial[0] = dot(mixed[0], temp_w[2 * channels :])
    partial[1] = dot(jnp.concatenate([mixed[0], mixed[1]], axis=1), temp_w[channels:])

    total = keep[core, mine] + core_in[mine].astype(F32)
    shift_total = shifts[1]
    for copy in direct_copies:
        copy.wait()
    for m in range(1, quads):
        total = total + quad_in[m].astype(F32)
        shift_total = shift_total + shifts_in[m]
    for n, device in enumerate(later):
        stage[2 * n] = total.astype(BF16)
        shifts[2 + n] = shift_total
        pair_copies = [
            remote(
                stage.at[2 * n], stage.at[2 * n + 1], fold_send.at[quads + n], fold_recv.at[quads + n], device
            ),
            remote(
                shifts.at[2 + n], shifts_in.at[quads + n],
                shift_send.at[quads + n], shift_recv.at[quads + n], device,
            ),
        ]
        for copy in pair_copies:
            copy.start()
        for copy in pair_copies:
            copy.wait()
        total = total + stage[2 * n + 1].astype(F32)
        shift_total = shift_total + shifts_in[quads + n]
    fold[core, mine] = total.astype(BF16)
    shift_out[...] = shift_total
    base = quads + len(later)
    shares = []

    def share_next():
        n = len(shares)
        if n < len(bits):
            known = fold.at[core, pl.ds(mine - lax.rem(mine, 2**n), 2**n)]
            copy = remote(
                known, known, fold_send.at[base + n], fold_recv.at[base + n], {bits[n][0]: bits[n][2]}
            )
            copy.start()
            shares.append(copy)

    share_next()

    centred = embed[...].astype(F32) - mean
    high = centred.astype(BF16)
    wide[0:pdim] = high
    wide[pdim:] = (centred - high.astype(F32)).astype(BF16)
    products = dot_t(wide[...], wide[...])
    gram = (
        products[:pdim, :pdim] + products[:pdim, pdim:]
        + products[pdim:, :pdim] + products[pdim:, pdim:]
    ) * (1.0 / wide_all)
    for i in range(3):
        piece = gram.astype(BF16)
        gram_out[i] = piece
        gram = gram - piece.astype(F32)

    @pl.when(has_before)
    def _():
        for copy in mix_copies[:rows]:
            copy.wait_recv()

    partial[0] = partial[0] + dot(before[0], temp_w[:channels])
    while done_phases[0] < phases:
        next_phase()

    @pl.when(has_before)
    def _():
        for copy in mix_copies[rows:]:
            copy.wait_recv()

    for f in range(frames):
        total = partial[f] + dot(before[1], temp_w[(1 - f) * channels : (2 - f) * channels])
        total = total + jnp.concatenate([feat[f, r].astype(F32) for r in range(rows)], axis=0)
        active = norm_silu(total).astype(BF16)
        term = dot(active[:columns], heads[PATCH * f]) + dot(active[columns:], heads[PATCH * f + 1])
        lat[...] = term if f == 0 else lat[...] + term
    tokens = columns // PATCH
    out_lane = lax.broadcasted_iota(jnp.int32, (tokens, LANES), 1)
    even = lat[pl.ds(0, tokens, stride=PATCH), :]
    odd = lat[pl.ds(1, tokens, stride=PATCH), :]
    gathered[row] = jnp.where(lax.rem(out_lane // latent, PATCH) == 0, even, odd).astype(BF16)
    sends = [
        remote(
            gathered.at[row], gathered.at[row], all_send.at[d], all_recv.at[d],
            {"rows": lax.rem(row + d, n_rows)},
        )
        for d in range(1, n_rows)
    ]
    for copy in sends:
        copy.start()
    for n in range(len(bits)):
        shares[n].wait()
        share_next()
    base += len(bits)
    widen = remote(fold.at[core], fold.at[core], fold_send.at[base], fold_recv.at[base], other_core)
    widen.start()

    @pl.when(has_above)
    def _():
        for copy in ups:
            copy.wait_send()

    @pl.when(has_below)
    def _():
        for copy in downs:
            copy.wait_send()

    @pl.when(has_after)
    def _():
        for copy in mix_copies:
            copy.wait_send()

    widen.wait()
    fold_out[...] = fold[...]
    for copy in sends:
        copy.wait()
    block_out[...] = gathered[...]


def project(n_rows, frames, block, fold, shift, gram, out, held, sems):
    pdim, width = fold.shape
    tokens = block.shape[1]
    lane = lax.broadcasted_iota(jnp.int32, (n_rows * tokens, LANES), 1)
    weights = jnp.concatenate([fold[...]] * frames, axis=0)
    quadratic = [jnp.concatenate([gram[i]] * frames, axis=0) for i in range(3)]
    everything = block[...].reshape(n_rows * tokens, LANES)
    parts = 4
    lines = n_rows * tokens // parts
    copies = []
    for f in range(frames):
        own = (lane >= f * pdim) & (lane < (f + 1) * pdim)
        packed = jnp.where(own, everything.astype(F32), 0.0)
        patches = packed.astype(BF16)
        for n in range(parts):
            mine = patches[n * lines : (n + 1) * lines]
            moved = dot(mine, quadratic[0]) + dot(mine, quadratic[1]) + dot(mine, quadratic[2])
            sides = packed[n * lines : (n + 1) * lines, f * pdim : (f + 1) * pdim]
            spread = jnp.maximum(jnp.sum(moved * sides, axis=-1, keepdims=True), 0.0)
            here = pl.ds((f * parts + n) * lines, lines)
            held[here] = dot(mine, weights) * lax.rsqrt(spread + EPS) + shift[...]
            copy = pltpu.make_async_copy(held.at[here], out.at[here], sems.at[f * parts + n])
            copy.start()
            copies.append(copy)
    for copy in copies:
        copy.wait()


def per_device(
    n_groups, n_tm, n_rows,
    features, spatial_weight, temporal_weight, head_weight, embed_weight, ada_scale, ada_shift, qkv_weight,
):
    frames, rows, columns, channels = features.shape
    depth, width = qkv_weight.shape
    pdim, wide_all = embed_weight.shape
    latent = head_weight.shape[1]
    split = n_groups == 2
    depth = depth // 2 if split else depth
    aligned = depth % LANES == 0
    quads = (2 if split else 1) * (2 if n_tm >= 4 else 1)
    later = max(n_tm.bit_length() - 3, 0)
    block_rows = pdim // (2 * quads)
    fold_shape = (2, quads, block_rows, width)
    part = embed_weight
    scale, shift = (v.reshape(wide_all // LANES, LANES) for v in (ada_scale, ada_shift))
    if not aligned:
        scale, shift = ada_scale[None], ada_shift[None]
        start = lax.axis_index("tm") * qkv_weight.shape[0]
        if split:
            start = start + lax.axis_index("groups") * depth
        scale, shift, part = (lax.dynamic_slice_in_dim(v, start, depth, axis=1) for v in (scale, shift, part))
    hbm = pl.BlockSpec(memory_space=pl.ANY)
    vmem = pl.BlockSpec(memory_space=pltpu.VMEM)
    tokens = columns // PATCH
    dma = pltpu.SemaphoreType.DMA
    block, fold, shift_row, gram = pl.pallas_call(
        functools.partial(encode, n_tm, n_rows, split, aligned),
        out_shape=(
            pltpu.VMEM((n_rows, tokens, LANES), BF16),
            pltpu.VMEM(fold_shape, BF16),
            pltpu.VMEM((1, width), F32),
            pltpu.VMEM((3, pdim, pdim), BF16),
        ),
        in_specs=[hbm] * 9,
        out_specs=(vmem, vmem, vmem, vmem),
        scratch_shapes=[
            pltpu.VMEM(features.shape, BF16),
            pltpu.VMEM((frames, 2, columns, channels), BF16),
            pltpu.VMEM((frames * columns, (rows + 2) * 3 * channels), BF16),
            pltpu.VMEM((9 * channels, channels), BF16),
            pltpu.VMEM((3 * channels, channels), BF16),
            pltpu.VMEM((latent, channels), BF16),
            pltpu.VMEM((pdim, wide_all), BF16),
            pltpu.VMEM((pdim, depth), BF16),
            pltpu.VMEM(scale.shape, BF16),
            pltpu.VMEM(shift.shape, BF16),
            pltpu.VMEM((2, wide_all // LANES, LANES), F32),
            pltpu.VMEM((2 * pdim, wide_all), BF16),
            pltpu.VMEM((depth, width), BF16),
            pltpu.VMEM((frames, rows * columns, channels), BF16),
            pltpu.VMEM((frames, rows * columns, channels), BF16),
            pltpu.VMEM((frames, rows * columns, channels), F32),
            pltpu.VMEM((columns, LANES), F32),
            pltpu.VMEM(fold_shape, BF16),
            pltpu.VMEM(fold_shape[1:], BF16),
            pltpu.VMEM(fold_shape, F32),
            pltpu.VMEM(fold_shape[1:], BF16),
            pltpu.VMEM(fold_shape[1:], BF16),
            pltpu.VMEM((max(2 * later, 1), block_rows, width), BF16),
            pltpu.VMEM(fold_shape, BF16),
            pltpu.VMEM((2 + later, 1, width), F32),
            pltpu.VMEM((quads + later, 1, width), F32),
            pltpu.VMEM((n_rows, tokens, LANES), BF16),
            pltpu.VMEM((PATCH * frames, channels, LANES), BF16),
            dma((9,)),
            dma((frames, 2)), dma((frames, 2)),
            dma((frames, rows)), dma((frames, rows)),
            dma((n_rows,)), dma((n_rows,)),
            dma((2 * quads + later + 1,)), dma((2 * quads + later + 1,)),
            dma((quads + later,)), dma((quads + later,)),
            pltpu.SemaphoreType.REGULAR((max(n_rows - 2, 1),)),
        ],
        compiler_params=pltpu.CompilerParams(
            collective_id=0, has_side_effects=True, vmem_limit_bytes=56 * 2**20
        ),
        name="encode",
    )(
        features,
        spatial_weight.reshape(9 * channels, channels),
        temporal_weight.reshape(3 * channels, channels),
        head_weight.T,
        embed_weight,
        part,
        scale,
        shift,
        qkv_weight,
    )
    count = frames * n_rows * tokens
    return pl.pallas_call(
        functools.partial(project, n_rows, frames),
        out_shape=jax.ShapeDtypeStruct((count, width), F32),
        in_specs=[vmem] * 4,
        out_specs=hbm,
        scratch_shapes=[pltpu.VMEM((count, width), F32), dma((4 * frames,))],
        compiler_params=pltpu.CompilerParams(vmem_limit_bytes=32 * 2**20),
        name="project",
    )(block, fold.reshape(pdim, width), shift_row, gram)


def solution(mesh):
    return jax.shard_map(
        functools.partial(per_device, mesh.shape["groups"], mesh.shape["tm"], mesh.shape["rows"]),
        mesh=mesh,
        in_specs=(
            P(("groups", "tm"), "rows", None, None),
            P(),
            P(),
            P(),
            P(),
            P(),
            P(),
            P("tm", "rows"),
        ),
        out_specs=P(("groups", "tm"), "rows"),
        check_vma=False,
    )
```

```python
import functools

import jax
import jax.numpy as jnp
from jax import lax
from jax.experimental import pallas as pl
from jax.experimental.pallas import tpu as pltpu
from jax.sharding import PartitionSpec as P

MESH = pl.DeviceIdType.MESH
PATCH = 2
LANES = 128
EPS = 1e-06
F32 = jnp.float32
BF16 = jnp.bfloat16


def dot(a, b):
    return jnp.dot(a, b, preferred_element_type=F32)


def dot_t(a, b):
    return lax.dot_general(a, b, (((1,), (1,)), ((), ())), preferred_element_type=F32)


def norm_silu(values):
    scaled = values * lax.rsqrt(jnp.mean(values * values, axis=-1, keepdims=True) + EPS)
    half = 0.5 * scaled
    return half + half * jnp.tanh(half)


def encode(
    n_tm, n_rows, split, aligned,
    features, spatial_hbm, temporal_hbm, head_hbm, embed_hbm, part_hbm, scale_hbm, shift_hbm, qkv_hbm,
    block_out, fold_out, shift_out, gram_out,
    feat, halo, taps, spat_w, temp_w, head_w, embed, part, scale_v, shift_v, vectors, wide, qkv_w,
    mixed, side, partial, lat, ahead, part_b, core_in, keep, cross, quad_in, stage, fold, shifts, shifts_in, gathered, heads,
    load_sem, halo_send, halo_recv, next_send, next_recv, mix_send, mix_recv,
    all_send, all_recv, ahead_send, ahead_recv, zero_send,
    fold_send, fold_recv, shift_send, shift_recv, relay, corner,
):
    group, tile, row = lax.axis_index("groups"), lax.axis_index("tm"), lax.axis_index("rows")
    frames, rows, columns, channels = features.shape
    depth, width = qkv_w.shape
    pdim, wide_all = embed.shape
    latent = head_w.shape[0]
    _, quads, block_rows, _ = fold.shape
    has_above, has_below = row > 0, row < n_rows - 1
    has_before, has_after = tile > 0, tile < n_tm - 1
    near = [({"rows": row - 1}, has_above), ({"rows": row + 1}, has_below)]
    count_rows = has_above.astype(jnp.int32) + has_below.astype(jnp.int32)
    count_tiles = has_before.astype(jnp.int32) + has_after.astype(jnp.int32)
    core = lax.rem(tile, 2)
    other_core = {"tm": tile + 1 - 2 * core}

    def flipped(bit):
        return tile + bit * (1 - 2 * lax.rem(tile // bit, 2))

    bits = [("tm", lax.rem(tile // 2, 2), flipped(2))] if n_tm >= 4 else []
    if split:
        bits.append(("groups", group, 1 - group))
    mine = sum((bit[1] * 2**n for n, bit in enumerate(bits)), 0)
    direct = []
    for mask in range(1, quads):
        chosen = [n for n in range(len(bits)) if mask >> n & 1]
        place = mine + sum(2**n * (1 - 2 * bits[n][1]) for n in chosen)
        direct.append(({bits[n][0]: bits[n][2] for n in chosen}, place))
    later = []
    step = 4
    while step < n_tm:
        later.append({"tm": flipped(step)})
        step *= 2
    partners = [other_core] + [device for device, _ in direct if len(device) == 1] + later

    def signal(sem, device):
        pl.semaphore_signal(sem, inc=1, device_id=device, device_id_type=MESH)

    barrier = pltpu.get_barrier_semaphore()
    for device in partners:
        signal(barrier, device)
    for device, there in near + [({"tm": tile - 1}, has_before), ({"tm": tile + 1}, has_after)]:

        @pl.when(there)
        def _():
            signal(barrier, device)

    def load(source, target, index):
        copy = pltpu.make_async_copy(source, target, load_sem.at[index])
        copy.start()
        return copy

    first = group * depth if split else 0
    load_feat = [load(features.at[f], feat.at[frames - f], 9 * f) for f in range(frames)]
    load_embed = load(embed_hbm, embed, 1)
    load_scale = load(scale_hbm, scale_v, 2)
    load_shift = load(shift_hbm, shift_v, 3)
    if not aligned:
        load_part = load(part_hbm, part, 4)
    load_qkv = load(qkv_hbm.at[pl.ds(pl.multiple_of(first, 16), depth)], qkv_w, 5)
    load_spat = load(spatial_hbm, spat_w, 6)
    load_temp = load(temporal_hbm, temp_w, 7)
    load_head = load(head_hbm, head_w, 8)

    def remote(source, target, send, recv, device):
        return pltpu.make_async_remote_copy(
            src_ref=source, dst_ref=target, send_sem=send, recv_sem=recv,
            device_id=device, device_id_type=MESH,
        )

    def up_copy(f):
        return remote(
            features.at[f, 0], halo.at[f, 1], halo_send.at[f, 0], halo_recv.at[f, 1], near[0][0]
        )

    def down_copy(f):
        return remote(
            features.at[f, rows - 1], halo.at[f, 0], halo_send.at[f, 1], halo_recv.at[f, 0], near[1][0]
        )

    next_copy = remote(features.at[0], feat.at[0], next_send.at[0], next_recv.at[0], {"tm": tile - 1})

    def mix_copy(f, r):
        lines = pl.ds(r * columns, columns)
        return remote(
            mixed.at[f, lines], side.at[1 - f, lines], mix_send.at[f, r], mix_recv.at[1 - f, r],
            {"tm": tile - 1 + 2 * f},
        )

    order = (core, 1 - core)
    forward = (core == 1, core == 0)
    neighboured = [
        jnp.logical_or(jnp.logical_and(up, has_after), jnp.logical_and(jnp.logical_not(up), has_before))
        for up in forward
    ]
    pl.semaphore_wait(barrier, len(partners) + count_rows + count_tiles)
    for f in order:
        @pl.when(has_above)
        def _():
            up_copy(f).start()

        @pl.when(has_below)
        def _():
            down_copy(f).start()

    @pl.when(has_before)
    def _():
        next_copy.start()

    phases = n_rows - 1
    done_phases = [0]

    def tell(phase):
        if phase < phases:
            for device, there in near:

                @pl.when(there)
                def _():
                    signal(relay.at[phase], device)

    def next_phase():
        phase = done_phases[0]
        if phase < phases:
            pl.semaphore_wait(relay.at[phase], count_rows)
            tell(phase + 1)
            done_phases[0] = phase + 1

    tell(0)
    if len(bits) == 2:
        signal(corner.at[0], {bits[1][0]: bits[1][2]})

    @pl.when(jnp.logical_not(has_above))
    def _():
        for f in range(frames):
            halo[f, 0] = jnp.zeros(halo.shape[2:], BF16)

    @pl.when(jnp.logical_not(has_below))
    def _():
        for f in range(frames):
            halo[f, 1] = jnp.zeros(halo.shape[2:], BF16)

    @pl.when(jnp.logical_not(has_before))
    def _():
        side[0] = jnp.zeros(side.shape[1:], BF16)

    @pl.when(jnp.logical_not(has_after))
    def _():
        side[1] = jnp.zeros(side.shape[1:], BF16)
        feat[0] = jnp.zeros(feat.shape[1:], BF16)

    span = 3 * channels
    column = lax.broadcasted_iota(jnp.int32, (columns, channels), 0)

    def spread_taps(values, place, frame):
        active = norm_silu(values.astype(F32))
        left = jnp.where(column == 0, 0.0, pltpu.roll(active, 1, 0))
        right = jnp.where(column == columns - 1, 0.0, pltpu.roll(active, columns - 1, 0))
        for k, shifted in enumerate((left, active, right)):
            taps[frame, :, pl.ds(place * span + k * channels, channels)] = shifted.astype(BF16)

    load_embed.wait()
    load_scale.wait()
    load_shift.wait()
    mean = jnp.mean(embed[...].astype(F32), axis=1, keepdims=True)
    if aligned:
        start = pl.multiple_of(tile * (wide_all // n_tm) + first, LANES)
        own = embed[:, pl.ds(start, depth)].astype(F32)
        vectors[0] = scale_v[...].astype(F32)
        vectors[1] = shift_v[...].astype(F32)
        at = start // LANES
        scale, shift = (
            jnp.concatenate([vectors[v, pl.ds(at + j, 1)] for j in range(depth // LANES)], axis=1)
            for v in range(2)
        )
    else:
        load_part.wait()
        own, scale, shift = part[...].astype(F32), scale_v[...].astype(F32), shift_v[...].astype(F32)
    scaled = ((own - mean) * (1.0 + scale)).astype(BF16)
    rows16 = lax.broadcasted_iota(jnp.int32, (16, depth), 0)
    shift16 = jnp.where(rows16 == 0, jnp.broadcast_to(shift, (16, depth)), 0.0).astype(BF16)
    lhs = jnp.concatenate([scaled, shift16], axis=0)
    load_qkv.wait()
    chunk = width // 3
    for n in range(3):
        cols = pl.ds(n * chunk, chunk)
        terms = dot(lhs, qkv_w[:, cols])
        shifts[0, :, cols] = terms[pdim : pdim + 1]
        for c in range(2):
            for b in range(quads):
                low = (c * quads + b) * block_rows
                piece = terms[low : low + block_rows]
                keep[c, b, :, cols] = piece
                part_b[c, b, :, cols] = piece.astype(BF16)

    core_copies = [
        remote(part_b.at[1 - core], core_in, fold_send.at[0], fold_recv.at[0], other_core),
        remote(shifts.at[0], shifts_in.at[0], shift_send.at[0], shift_recv.at[0], other_core),
    ]
    for copy in core_copies:
        copy.start()

    for copy in load_feat:
        copy.wait()
    for f in range(frames):
        for r in range(rows):
            spread_taps(feat[frames - f, r], r + 1, f)
    load_spat.wait()
    inner = taps[:, :, span : 3 * span].reshape(frames * columns, 2 * span)
    direct_copies = []
    for r in range(rows):
        total = dot(inner, spat_w[(1 - r) * span : (3 - r) * span])
        for f in range(frames):
            partial[f, pl.ds(r * columns, columns)] = total[f * columns : (f + 1) * columns]
        if r == 0:
            for copy in core_copies:
                copy.wait()
            shifts[1] = shifts[0] + shifts_in[0]
            for b in range(quads):
                cross[b] = (keep[core, b] + core_in[b].astype(F32)).astype(BF16)
            for m, (device, place) in enumerate(direct, 1):
                direct_copies += [
                    remote(cross.at[place], quad_in.at[m], fold_send.at[m], fold_recv.at[m], device),
                    remote(shifts.at[1], shifts_in.at[m], shift_send.at[m], shift_recv.at[m], device),
                ]
            if len(bits) == 2:
                pl.semaphore_wait(corner.at[0], 1)
            for copy in direct_copies:
                copy.start()
    next_phase()

    def end_direct():
        total = keep[core, mine] + core_in[mine].astype(F32)
        shift_total = shifts[1]
        for copy in direct_copies:
            copy.wait()
        for m in range(1, quads):
            total = total + quad_in[m].astype(F32)
            shift_total = shift_total + shifts_in[m]
        for n, device in enumerate(later):
            stage[2 * n] = total.astype(BF16)
            shifts[2 + n] = shift_total
            pair_copies = [
                remote(
                    stage.at[2 * n], stage.at[2 * n + 1],
                    fold_send.at[quads + n], fold_recv.at[quads + n], device,
                ),
                remote(
                    shifts.at[2 + n], shifts_in.at[quads + n],
                    shift_send.at[quads + n], shift_recv.at[quads + n], device,
                ),
            ]
            for copy in pair_copies:
                copy.start()
            for copy in pair_copies:
                copy.wait()
            total = total + stage[2 * n + 1].astype(F32)
            shift_total = shift_total + shifts_in[quads + n]
        fold[core, mine] = total.astype(BF16)
        shift_out[...] = shift_total
        for copy in share_copies:
            copy.start()

    base = quads + len(later)
    share_copies = [
        remote(
            fold.at[core, mine], fold.at[core, mine], fold_send.at[base + m], fold_recv.at[base + m], device
        )
        for m, (device, _) in enumerate(direct)
    ]
    base += len(share_copies)

    load_head.wait()

    def place_heads():
        lane = lax.broadcasted_iota(jnp.int32, (latent, LANES), 1)
        latent_lane = lax.broadcasted_iota(jnp.int32, (latent, LANES), 0)
        pair = PATCH * latent
        for a in range(PATCH):
            low = a * pair
            pick = (lane >= low) & (lane < low + pair) & (lax.rem(lane, latent) == latent_lane)
            spread_head = lax.dot_general(
                head_w[...], jnp.where(pick, 1.0, 0.0).astype(BF16), (((0,), (0,)), ((), ())),
                preferred_element_type=F32,
            )
            heads[a] = spread_head.astype(BF16)

    def finish_frame(f, there):
        @pl.when(has_above)
        def _():
            down_copy(f).wait_recv()

        @pl.when(has_below)
        def _():
            up_copy(f).wait_recv()

        spread_taps(halo[f, 0], 0, f)
        spread_taps(halo[f, 1], rows + 1, f)
        for r, (place, weights) in enumerate(
            ((0, spat_w[0:span]), (3 * span, spat_w[2 * span : 3 * span]))
        ):
            lines = pl.ds(r * columns, columns)
            total = partial[f, lines] + dot(taps[f, :, pl.ds(place, span)], weights)
            mixed[f, lines] = norm_silu(total).astype(BF16)

            @pl.when(there)
            def _():
                mix_copy(f, r).start()

    @pl.when(core == 0)
    def _():
        place_heads()

    finish_frame(order[0], neighboured[0])
    next_phase()
    finish_frame(order[1], neighboured[1])

    @pl.when(core == 1)
    def _():
        place_heads()

    load_temp.wait()
    own_frames = jnp.concatenate([mixed[0], mixed[1]], axis=1)
    partial[0] = dot(own_frames, temp_w[0:2].reshape(2 * channels, channels))
    partial[1] = dot(own_frames, temp_w[1:3].reshape(2 * channels, channels))

    end_direct()

    while done_phases[0] < phases:
        next_phase()

    @pl.when(has_after)
    def _():
        next_copy.wait_recv()

    tokens = columns // PATCH
    out_lane = lax.broadcasted_iota(jnp.int32, (tokens, LANES), 1)
    even_lane = lax.rem(out_lane // latent, PATCH) == 0

    def patches_of(total, residual):
        total = total + jnp.concatenate([feat[residual, r].astype(F32) for r in range(rows)], axis=0)
        active = norm_silu(total).astype(BF16)
        lat[...] = dot(active[:columns], heads[0]) + dot(active[columns:], heads[1])
        even = lat[pl.ds(0, tokens, stride=PATCH), :]
        odd = lat[pl.ds(1, tokens, stride=PATCH), :]
        return jnp.where(even_lane, even, odd).astype(BF16)

    def away(d):
        return lax.rem(row + d, n_rows)

    sends = [
        remote(
            gathered.at[1, row], gathered.at[1, row], all_send.at[d], all_recv.at[d], {"rows": away(d)}
        )
        for d in range(1, n_rows)
    ]
    ahead_sends = [
        remote(
            ahead, gathered.at[0, row], ahead_send.at[d], ahead_recv.at[d],
            {"tm": tile + 1, "rows": away(d)},
        )
        for d in range(n_rows)
    ]
    zero_sends = [
        remote(
            gathered.at[0, row], gathered.at[0, row], zero_send.at[d], ahead_recv.at[d], {"rows": away(d)}
        )
        for d in range(1, n_rows)
    ]

    is_first = tile == 0

    @pl.when(is_first)
    def _():
        gathered[0, row] = patches_of(dot(mixed[0], temp_w[2]), frames)
        for copy in zero_sends:
            copy.start()

    slots = jnp.where(is_first, 1, core)
    for s, own in ((slots, slots == 1), (1 - slots, slots == 0)):
        filled = jnp.logical_or(
            jnp.logical_and(own, has_before), jnp.logical_and(jnp.logical_not(own), has_after)
        )

        @pl.when(filled)
        def _():
            for r in range(rows):
                mix_copy(s, r).wait_recv()

        patches = patches_of(partial[s] + dot(side[1 - s], temp_w[2 * (1 - s)]), s)

        @pl.when(own)
        def _():
            gathered[1, row] = patches
            for copy in sends:
                copy.start()

        @pl.when(jnp.logical_and(jnp.logical_not(own), has_after))
        def _():
            ahead[...] = patches
            for copy in ahead_sends:
                copy.start()

    for copy in share_copies:
        copy.wait()
    widen = remote(fold.at[core], fold.at[core], fold_send.at[base], fold_recv.at[base], other_core)
    widen.start()

    centred = embed[...].astype(F32) - mean
    high = centred.astype(BF16)
    wide[0:pdim] = high
    wide[pdim:] = (centred - high.astype(F32)).astype(BF16)
    products = dot_t(wide[...], wide[...])
    gram = (
        products[:pdim, :pdim] + products[:pdim, pdim:]
        + products[pdim:, :pdim] + products[pdim:, pdim:]
    ) * (1.0 / wide_all)
    for i in range(3):
        piece = gram.astype(BF16)
        gram_out[i] = piece
        gram = gram - piece.astype(F32)

    @pl.when(has_above)
    def _():
        for f in range(frames):
            up_copy(f).wait_send()

    @pl.when(has_below)
    def _():
        for f in range(frames):
            down_copy(f).wait_send()

    @pl.when(has_before)
    def _():
        next_copy.wait_send()
        for r in range(rows):
            mix_copy(0, r).wait_send()

    @pl.when(has_after)
    def _():
        for r in range(rows):
            mix_copy(1, r).wait_send()
        for copy in ahead_sends:
            copy.wait_send()

    @pl.when(is_first)
    def _():
        for copy in zero_sends:
            copy.wait_send()

    widen.wait()
    fold_out[...] = fold[...]
    for copy in sends:
        copy.wait()

    @pl.when(has_before)
    def _():
        ahead_sends[0].wait_recv()

    for copy in ahead_sends[1:]:
        copy.wait_recv()
    block_out[...] = gathered[...]


def project(block, fold, shift, gram, out, held, sems):
    pdim, width = fold.shape
    frames, n_rows, tokens, _ = block.shape
    parts = 4
    lines = n_rows * tokens // parts
    copies = []
    for f in range(frames):
        patches = block[f].reshape(n_rows * tokens, LANES)[:, :pdim]
        for n in range(parts):
            own = patches[n * lines : (n + 1) * lines]
            moved = dot(own, gram[0]) + dot(own, gram[1]) + dot(own, gram[2])
            spread = jnp.maximum(jnp.sum(moved * own.astype(F32), axis=-1, keepdims=True), 0.0)
            here = pl.ds((f * parts + n) * lines, lines)
            held[here] = dot(own, fold[...]) * lax.rsqrt(spread + EPS) + shift[...]
            copy = pltpu.make_async_copy(held.at[here], out.at[here], sems.at[f * parts + n])
            copy.start()
            copies.append(copy)
    for copy in copies:
        copy.wait()


def per_device(
    n_groups, n_tm, n_rows,
    features, spatial_weight, temporal_weight, head_weight, embed_weight, ada_scale, ada_shift, qkv_weight,
):
    frames, rows, columns, channels = features.shape
    depth, width = qkv_weight.shape
    pdim, wide_all = embed_weight.shape
    latent = head_weight.shape[1]
    split = n_groups == 2
    depth = depth // 2 if split else depth
    aligned = depth % LANES == 0
    quads = (2 if split else 1) * (2 if n_tm >= 4 else 1)
    later = max(n_tm.bit_length() - 3, 0)
    block_rows = pdim // (2 * quads)
    fold_shape = (2, quads, block_rows, width)
    part = embed_weight
    scale, shift = (v.reshape(wide_all // LANES, LANES) for v in (ada_scale, ada_shift))
    if not aligned:
        scale, shift = ada_scale[None], ada_shift[None]
        start = lax.axis_index("tm") * qkv_weight.shape[0]
        if split:
            start = start + lax.axis_index("groups") * depth
        scale, shift, part = (lax.dynamic_slice_in_dim(v, start, depth, axis=1) for v in (scale, shift, part))
    hbm = pl.BlockSpec(memory_space=pl.ANY)
    vmem = pl.BlockSpec(memory_space=pltpu.VMEM)
    tokens = columns // PATCH
    dma = pltpu.SemaphoreType.DMA
    block, fold, shift_row, gram = pl.pallas_call(
        functools.partial(encode, n_tm, n_rows, split, aligned),
        out_shape=(
            pltpu.VMEM((frames, n_rows, tokens, LANES), BF16),
            pltpu.VMEM(fold_shape, BF16),
            pltpu.VMEM((1, width), F32),
            pltpu.VMEM((3, pdim, pdim), BF16),
        ),
        in_specs=[hbm] * 9,
        out_specs=(vmem, vmem, vmem, vmem),
        scratch_shapes=[
            pltpu.VMEM((frames + 1, rows, columns, channels), BF16),
            pltpu.VMEM((frames, 2, columns, channels), BF16),
            pltpu.VMEM((frames, columns, (rows + 2) * 3 * channels), BF16),
            pltpu.VMEM((9 * channels, channels), BF16),
            pltpu.VMEM((3, channels, channels), BF16),
            pltpu.VMEM((latent, channels), BF16),
            pltpu.VMEM((pdim, wide_all), BF16),
            pltpu.VMEM((pdim, depth), BF16),
            pltpu.VMEM(scale.shape, BF16),
            pltpu.VMEM(shift.shape, BF16),
            pltpu.VMEM((2, wide_all // LANES, LANES), F32),
            pltpu.VMEM((2 * pdim, wide_all), BF16),
            pltpu.VMEM((depth, width), BF16),
            pltpu.VMEM((frames, rows * columns, channels), BF16),
            pltpu.VMEM((frames, rows * columns, channels), BF16),
            pltpu.VMEM((frames, rows * columns, channels), F32),
            pltpu.VMEM((columns, LANES), F32),
            pltpu.VMEM((tokens, LANES), BF16),
            pltpu.VMEM(fold_shape, BF16),
            pltpu.VMEM(fold_shape[1:], BF16),
            pltpu.VMEM(fold_shape, F32),
            pltpu.VMEM(fold_shape[1:], BF16),
            pltpu.VMEM(fold_shape[1:], BF16),
            pltpu.VMEM((max(2 * later, 1), block_rows, width), BF16),
            pltpu.VMEM(fold_shape, BF16),
            pltpu.VMEM((2 + later, 1, width), F32),
            pltpu.VMEM((quads + later, 1, width), F32),
            pltpu.VMEM((frames, n_rows, tokens, LANES), BF16),
            pltpu.VMEM((PATCH, channels, LANES), BF16),
            dma((10,)),
            dma((frames, 2)), dma((frames, 2)),
            dma((1,)), dma((1,)),
            dma((frames, rows)), dma((frames, rows)),
            dma((n_rows,)), dma((n_rows,)),
            dma((n_rows,)), dma((n_rows,)), dma((n_rows,)),
            dma((2 * quads + later + 1,)), dma((2 * quads + later + 1,)),
            dma((quads + later,)), dma((quads + later,)),
            pltpu.SemaphoreType.REGULAR((max(n_rows - 1, 1),)),
            pltpu.SemaphoreType.REGULAR((1,)),
        ],
        compiler_params=pltpu.CompilerParams(
            collective_id=0, has_side_effects=True, vmem_limit_bytes=56 * 2**20
        ),
        name="encode",
    )(
        features,
        spatial_weight.reshape(9 * channels, channels),
        temporal_weight,
        head_weight.T,
        embed_weight,
        part,
        scale,
        shift,
        qkv_weight,
    )
    count = frames * n_rows * tokens
    return pl.pallas_call(
        project,
        out_shape=jax.ShapeDtypeStruct((count, width), F32),
        in_specs=[vmem] * 4,
        out_specs=hbm,
        scratch_shapes=[pltpu.VMEM((count, width), F32), dma((4 * frames,))],
        compiler_params=pltpu.CompilerParams(vmem_limit_bytes=32 * 2**20),
        name="project",
    )(block, fold.reshape(pdim, width), shift_row, gram)


def solution(mesh):
    return jax.shard_map(
        functools.partial(per_device, mesh.shape["groups"], mesh.shape["tm"], mesh.shape["rows"]),
        mesh=mesh,
        in_specs=(
            P(("groups", "tm"), "rows", None, None),
            P(),
            P(),
            P(),
            P(),
            P(),
            P(),
            P("tm", "rows"),
        ),
        out_specs=P(("groups", "tm"), "rows"),
        check_vma=False,
    )
```

```python
import functools

import jax
import jax.numpy as jnp
from jax import lax
from jax.experimental import pallas as pl
from jax.experimental.pallas import tpu as pltpu
from jax.sharding import PartitionSpec as P

MESH = pl.DeviceIdType.MESH
PATCH = 2
LANES = 128
EPS = 1e-06
F32 = jnp.float32
BF16 = jnp.bfloat16


def dot(a, b):
    return jnp.dot(a, b, preferred_element_type=F32)


def dot_t(a, b):
    return lax.dot_general(a, b, (((1,), (1,)), ((), ())), preferred_element_type=F32)


def norm_silu(values):
    scaled = values * lax.rsqrt(jnp.mean(values * values, axis=-1, keepdims=True) + EPS)
    half = 0.5 * scaled
    return half + half * jnp.tanh(half)


def encode(
    n_tm, n_rows, split, aligned,
    features, spatial_hbm, temporal_hbm, head_hbm, embed_hbm, part_hbm, scale_hbm, shift_hbm, qkv_hbm,
    block_out, fold_out, shift_out, gram_out,
    feat, halo, taps, spat_w, temp_w, head_w, embed, part, scale_v, shift_v, vectors, wide, qkv_w,
    mixed, side, bracket, partial, lat, ahead, part_b, core_in, keep, cross, quad_in, stage, fold, shifts, shifts_in, gathered, heads,
    load_sem, halo_send, halo_recv, mix_send, mix_recv,
    all_send, all_recv, ahead_send, ahead_recv, zero_send,
    fold_send, fold_recv, shift_send, shift_recv, relay, corner,
):
    group, tile, row = lax.axis_index("groups"), lax.axis_index("tm"), lax.axis_index("rows")
    frames, rows, columns, channels = features.shape
    depth, width = qkv_w.shape
    pdim, wide_all = embed.shape
    latent = head_w.shape[0]
    _, quads, block_rows, _ = fold.shape
    has_above, has_below = row > 0, row < n_rows - 1
    has_before, has_after = tile > 0, tile < n_tm - 1
    near = [({"rows": row - 1}, has_above), ({"rows": row + 1}, has_below)]
    count_rows = has_above.astype(jnp.int32) + has_below.astype(jnp.int32)
    count_tiles = has_before.astype(jnp.int32) + has_after.astype(jnp.int32)
    core = lax.rem(tile, 2)
    other_core = {"tm": tile + 1 - 2 * core}

    def flipped(bit):
        return tile + bit * (1 - 2 * lax.rem(tile // bit, 2))

    bits = [("tm", lax.rem(tile // 2, 2), flipped(2))] if n_tm >= 4 else []
    if split:
        bits.append(("groups", group, 1 - group))
    mine = sum((bit[1] * 2**n for n, bit in enumerate(bits)), 0)
    direct = []
    for mask in range(1, quads):
        chosen = [n for n in range(len(bits)) if mask >> n & 1]
        place = mine + sum(2**n * (1 - 2 * bits[n][1]) for n in chosen)
        direct.append(({bits[n][0]: bits[n][2] for n in chosen}, place))
    later = []
    step = 4
    while step < n_tm:
        later.append({"tm": flipped(step)})
        step *= 2
    partners = [other_core] + [device for device, _ in direct if len(device) == 1] + later

    def signal(sem, device):
        pl.semaphore_signal(sem, inc=1, device_id=device, device_id_type=MESH)

    barrier = pltpu.get_barrier_semaphore()
    for device in partners:
        signal(barrier, device)
    for device, there in near + [({"tm": tile - 1}, has_before), ({"tm": tile + 1}, has_after)]:

        @pl.when(there)
        def _():
            signal(barrier, device)

    def load(source, target, index):
        copy = pltpu.make_async_copy(source, target, load_sem.at[index])
        copy.start()
        return copy

    first = group * depth if split else 0
    load_feat = load(features, feat, 0)
    load_embed = load(embed_hbm, embed, 1)
    load_scale = load(scale_hbm, scale_v, 2)
    load_shift = load(shift_hbm, shift_v, 3)
    if not aligned:
        load_part = load(part_hbm, part, 9)
    load_qkv = load(qkv_hbm.at[pl.ds(pl.multiple_of(first, 16), depth)], qkv_w, 4)
    span = 3 * channels
    load_spat = [
        load(spatial_hbm.at[lines], spat_w.at[lines], index)
        for lines, index in ((pl.ds(span, 2 * span), 5), (pl.ds(0, span), 8))
    ]
    load_temp = load(temporal_hbm, temp_w, 6)
    load_head = load(head_hbm, head_w, 7)

    def remote(source, target, send, recv, device):
        return pltpu.make_async_remote_copy(
            src_ref=source, dst_ref=target, send_sem=send, recv_sem=recv,
            device_id=device, device_id_type=MESH,
        )

    def up_copy(f):
        return remote(
            features.at[f, 0], halo.at[f, 1], halo_send.at[0], halo_recv.at[f, 1], near[0][0]
        )

    def down_copy(f):
        return remote(
            features.at[f, rows - 1], halo.at[f, 0], halo_send.at[1], halo_recv.at[f, 0], near[1][0]
        )

    onward = remote(mixed.at[1], side.at[0], mix_send.at[1], mix_recv.at[0], {"tm": tile + 1})
    back = remote(bracket, side.at[1], mix_send.at[0], mix_recv.at[1], {"tm": tile - 1})

    order = (core, 1 - core)
    pl.semaphore_wait(barrier, len(partners) + count_rows + count_tiles)
    for f in order:
        @pl.when(has_above)
        def _():
            up_copy(f).start()

        @pl.when(has_below)
        def _():
            down_copy(f).start()

    phases = n_rows - 1
    done_phases = [0]

    def tell(phase):
        if phase < phases:
            for device, there in near:

                @pl.when(there)
                def _():
                    signal(relay.at[phase], device)

    def next_phase():
        phase = done_phases[0]
        if phase < phases:
            pl.semaphore_wait(relay.at[phase], count_rows)
            tell(phase + 1)
            done_phases[0] = phase + 1

    tell(0)
    if len(bits) == 2:
        signal(corner.at[0], {bits[1][0]: bits[1][2]})

    @pl.when(jnp.logical_not(has_above))
    def _():
        for f in range(frames):
            halo[f, 0] = jnp.zeros(halo.shape[2:], BF16)

    @pl.when(jnp.logical_not(has_below))
    def _():
        for f in range(frames):
            halo[f, 1] = jnp.zeros(halo.shape[2:], BF16)

    @pl.when(jnp.logical_not(has_before))
    def _():
        side[0] = jnp.zeros(side.shape[1:], BF16)

    column = lax.broadcasted_iota(jnp.int32, (columns, channels), 0)

    def spread_taps(values, place, frame):
        active = norm_silu(values.astype(F32))
        left = jnp.where(column == 0, 0.0, pltpu.roll(active, 1, 0))
        right = jnp.where(column == columns - 1, 0.0, pltpu.roll(active, columns - 1, 0))
        for k, shifted in enumerate((left, active, right)):
            taps[frame, :, pl.ds(place * span + k * channels, channels)] = shifted.astype(BF16)

    load_feat.wait()
    for f in range(frames):
        for r in range(rows):
            spread_taps(feat[f, r], r + 1, f)

    load_embed.wait()
    load_scale.wait()
    load_shift.wait()
    mean = jnp.mean(embed[...].astype(F32), axis=1, keepdims=True)
    if aligned:
        start = pl.multiple_of(tile * (wide_all // n_tm) + first, LANES)
        own = embed[:, pl.ds(start, depth)].astype(F32)
        vectors[0] = scale_v[...].astype(F32)
        vectors[1] = shift_v[...].astype(F32)
        at = start // LANES
        scale, shift = (
            jnp.concatenate([vectors[v, pl.ds(at + j, 1)] for j in range(depth // LANES)], axis=1)
            for v in range(2)
        )
    else:
        load_part.wait()
        own, scale, shift = part[...].astype(F32), scale_v[...].astype(F32), shift_v[...].astype(F32)
    scaled = (own - mean) * (1.0 + scale)
    upper = scaled.astype(BF16)
    lower = (scaled - upper.astype(F32)).astype(BF16)
    rows16 = lax.broadcasted_iota(jnp.int32, (16, depth), 0)
    shift16 = jnp.where(rows16 == 0, jnp.broadcast_to(shift, (16, depth)), 0.0).astype(BF16)
    lhs = jnp.concatenate([upper, lower, shift16], axis=0)
    load_qkv.wait()
    chunk = width // 3
    for n in range(3):
        cols = pl.ds(n * chunk, chunk)
        terms = dot(lhs, qkv_w[:, cols])
        shifts[0, :, cols] = terms[2 * pdim : 2 * pdim + 1]
        terms = terms[:pdim] + terms[pdim : 2 * pdim]
        for c in range(2):
            for b in range(quads):
                low = (c * quads + b) * block_rows
                piece = terms[low : low + block_rows]
                keep[c, b, :, cols] = piece
                part_b[c, b, :, cols] = piece.astype(BF16)

    core_copies = [
        remote(part_b.at[1 - core], core_in, fold_send.at[0], fold_recv.at[0], other_core),
        remote(shifts.at[0], shifts_in.at[0], shift_send.at[0], shift_recv.at[0], other_core),
    ]
    for copy in core_copies:
        copy.start()

    inner = taps[:, :, span : 3 * span].reshape(frames * columns, 2 * span)
    direct_copies = []
    for r in range(rows):
        load_spat[r].wait()
        total = dot(inner, spat_w[(1 - r) * span : (3 - r) * span])
        for f in range(frames):
            partial[f, pl.ds(r * columns, columns)] = total[f * columns : (f + 1) * columns]
        if r == 0:
            for copy in core_copies:
                copy.wait()
            shifts[1] = shifts[0] + shifts_in[0]
            for b in range(quads):
                cross[b] = (keep[core, b] + core_in[b].astype(F32)).astype(BF16)
            for m, (device, place) in enumerate(direct, 1):
                direct_copies += [
                    remote(cross.at[place], quad_in.at[m], fold_send.at[1], fold_recv.at[1], device),
                    remote(shifts.at[1], shifts_in.at[m], shift_send.at[1], shift_recv.at[1], device),
                ]
            if len(bits) == 2:
                pl.semaphore_wait(corner.at[0], 1)
            for copy in direct_copies:
                copy.start()
    next_phase()

    def end_direct():
        total = keep[core, mine] + core_in[mine].astype(F32)
        shift_total = shifts[1]
        if direct:
            device = direct[0][0]
            for copy in (
                remote(quad_in.at[1:], quad_in.at[1:], fold_send.at[1], fold_recv.at[1], device),
                remote(
                    shifts_in.at[1:quads], shifts_in.at[1:quads], shift_send.at[1], shift_recv.at[1], device
                ),
            ):
                copy.wait()
        for m in range(1, quads):
            total = total + quad_in[m].astype(F32)
            shift_total = shift_total + shifts_in[m]
        for n, device in enumerate(later):
            stage[2 * n] = total.astype(BF16)
            shifts[2 + n] = shift_total
            pair_copies = [
                remote(
                    stage.at[2 * n], stage.at[2 * n + 1],
                    fold_send.at[2 + n], fold_recv.at[2 + n], device,
                ),
                remote(
                    shifts.at[2 + n], shifts_in.at[quads + n],
                    shift_send.at[2 + n], shift_recv.at[2 + n], device,
                ),
            ]
            for copy in pair_copies:
                copy.start()
            for copy in pair_copies:
                copy.wait()
            total = total + stage[2 * n + 1].astype(F32)
            shift_total = shift_total + shifts_in[quads + n]
        fold[core, mine] = total.astype(BF16)
        shift_out[...] = shift_total
        for copy in share_copies:
            copy.start()

    base = 2 + len(later)
    share_copies = [
        remote(fold.at[core, mine], fold.at[core, mine], fold_send.at[base], fold_recv.at[base], device)
        for device, _ in direct
    ]

    load_head.wait()

    def place_heads():
        lane = lax.broadcasted_iota(jnp.int32, (latent, LANES), 1)
        latent_lane = lax.broadcasted_iota(jnp.int32, (latent, LANES), 0)
        pair = PATCH * latent
        for a in range(PATCH):
            low = a * pair
            pick = (lane >= low) & (lane < low + pair) & (lax.rem(lane, latent) == latent_lane)
            spread_head = lax.dot_general(
                head_w[...], jnp.where(pick, 1.0, 0.0).astype(BF16), (((0,), (0,)), ((), ())),
                preferred_element_type=F32,
            )
            heads[a] = spread_head.astype(BF16)

    load_temp.wait()

    def finish_frame(f):
        @pl.when(has_above)
        def _():
            down_copy(f).wait_recv()

        @pl.when(has_below)
        def _():
            up_copy(f).wait_recv()

        spread_taps(halo[f, 0], 0, f)
        spread_taps(halo[f, 1], rows + 1, f)
        totals = []
        for r, (place, weights) in enumerate(
            ((0, spat_w[0:span]), (3 * span, spat_w[2 * span : 3 * span]))
        ):
            lines = pl.ds(r * columns, columns)
            totals.append(partial[f, lines] + dot(taps[f, :, pl.ds(place, span)], weights))
        mixed[f] = norm_silu(jnp.concatenate(totals, axis=0)).astype(BF16)

        @pl.when(jnp.logical_and(f == 1, has_after))
        def _():
            onward.start()

        @pl.when(f == 0)
        def _():
            residual = jnp.concatenate([feat[0, r].astype(F32) for r in range(rows)], axis=0)
            bracket[...] = (dot(mixed[0], temp_w[2]) + residual).astype(BF16)

            @pl.when(has_before)
            def _():
                back.start()

    @pl.when(core == 0)
    def _():
        place_heads()

    finish_frame(order[0])
    next_phase()
    finish_frame(order[1])

    @pl.when(core == 1)
    def _():
        place_heads()

    own_frames = jnp.concatenate([mixed[0], mixed[1]], axis=1)
    partial[0] = dot(own_frames, temp_w[0:2].reshape(2 * channels, channels))
    partial[1] = dot(own_frames, temp_w[1:3].reshape(2 * channels, channels))

    early = 2 * row < n_rows

    @pl.when(early)
    def _():
        end_direct()

    while done_phases[0] < phases:
        next_phase()

    tokens = columns // PATCH
    out_lane = lax.broadcasted_iota(jnp.int32, (tokens, LANES), 1)
    even_lane = lax.rem(out_lane // latent, PATCH) == 0

    def patches_of(total):
        active = norm_silu(total).astype(BF16)
        lat[...] = dot(active[:columns], heads[0]) + dot(active[columns:], heads[1])
        even = lat[pl.ds(0, tokens, stride=PATCH), :]
        odd = lat[pl.ds(1, tokens, stride=PATCH), :]
        return jnp.where(even_lane, even, odd).astype(BF16)

    def away(d):
        return lax.rem(row + d, n_rows)

    sends = [
        remote(
            gathered.at[1, row], gathered.at[1, row], all_send.at[0], all_recv.at[0], {"rows": away(d)}
        )
        for d in range(1, n_rows)
    ]
    ahead_sends = [
        remote(
            ahead, gathered.at[0, row], ahead_send.at[0], ahead_recv.at[0],
            {"tm": tile + 1, "rows": away(d)},
        )
        for d in range(n_rows)
    ]
    zero_sends = [
        remote(
            gathered.at[0, row], gathered.at[0, row], zero_send.at[0], ahead_recv.at[0], {"rows": away(d)}
        )
        for d in range(1, n_rows)
    ]

    is_first = tile == 0

    @pl.when(is_first)
    def _():
        gathered[0, row] = patches_of(bracket[...].astype(F32))
        for copy in zero_sends:
            copy.start()

    def last_frame():
        @pl.when(has_before)
        def _():
            onward.wait_recv()

        residual = jnp.concatenate([feat[1, r].astype(F32) for r in range(rows)], axis=0)
        gathered[1, row] = patches_of(partial[1] + dot(side[0], temp_w[0]) + residual)
        for copy in sends:
            copy.start()

    last_first = jnp.logical_or(is_first, core == 1)
    late = jnp.logical_not(early)

    @pl.when(last_first)
    def _():
        last_frame()

    @pl.when(jnp.logical_and(last_first, late))
    def _():
        end_direct()

    @pl.when(has_after)
    def _():
        back.wait_recv()
        ahead[...] = patches_of(partial[0] + side[1].astype(F32))
        for copy in ahead_sends:
            copy.start()

    @pl.when(jnp.logical_and(jnp.logical_not(last_first), late))
    def _():
        end_direct()

    @pl.when(jnp.logical_not(last_first))
    def _():
        last_frame()

    if direct:
        others = fold.at[core, 0 : quads - 1]
        remote(others, others, fold_send.at[base], fold_recv.at[base], direct[0][0]).wait()
    base += 1
    widen = remote(fold.at[core], fold.at[core], fold_send.at[base], fold_recv.at[base], other_core)
    widen.start()

    centred = embed[...].astype(F32) - mean
    high = centred.astype(BF16)
    wide[0:pdim] = high
    wide[pdim:] = (centred - high.astype(F32)).astype(BF16)
    products = dot_t(wide[...], wide[...])
    gram = (
        products[:pdim, :pdim] + products[:pdim, pdim:]
        + products[pdim:, :pdim] + products[pdim:, pdim:]
    ) * (1.0 / wide_all)
    for i in range(3):
        piece = gram.astype(BF16)
        gram_out[i] = piece
        gram = gram - piece.astype(F32)

    @pl.when(has_above)
    def _():
        edge = features.at[:, 0]
        remote(edge, halo.at[:, 1], halo_send.at[0], halo_recv.at[0, 1], near[0][0]).wait_send()

    @pl.when(has_below)
    def _():
        edge = features.at[:, rows - 1]
        remote(edge, halo.at[:, 0], halo_send.at[1], halo_recv.at[0, 0], near[1][0]).wait_send()

    @pl.when(has_before)
    def _():
        back.wait_send()

    def all_of(frame, count, send, recv):
        several = gathered.at[frame, 0:count]
        return remote(several, several, send.at[0], recv.at[0], other_core)

    @pl.when(has_after)
    def _():
        onward.wait_send()
        all_of(0, n_rows, ahead_send, ahead_recv).wait_send()

    if n_rows > 1:

        @pl.when(is_first)
        def _():
            all_of(0, n_rows - 1, zero_send, ahead_recv).wait_send()

    widen.wait()
    fold_out[...] = fold[...]
    if n_rows > 1:
        all_of(1, n_rows - 1, all_send, all_recv).wait()

        @pl.when(is_first)
        def _():
            all_of(0, n_rows - 1, zero_send, ahead_recv).wait_recv()

    @pl.when(has_before)
    def _():
        all_of(0, n_rows, ahead_send, ahead_recv).wait_recv()

    block_out[...] = gathered[...]


def project(block, fold, shift, gram, out, held, sems):
    pdim, width = fold.shape
    frames, n_rows, tokens, _ = block.shape
    parts = 4
    lines = n_rows * tokens // parts
    copies = []
    for f in range(frames):
        patches = block[f].reshape(n_rows * tokens, LANES)[:, :pdim]
        for n in range(parts):
            own = patches[n * lines : (n + 1) * lines]
            moved = dot(own, gram[0]) + dot(own, gram[1]) + dot(own, gram[2])
            spread = jnp.maximum(jnp.sum(moved * own.astype(F32), axis=-1, keepdims=True), 0.0)
            here = pl.ds((f * parts + n) * lines, lines)
            held[here] = dot(own, fold[...]) * lax.rsqrt(spread + EPS) + shift[...]
            copy = pltpu.make_async_copy(held.at[here], out.at[here], sems.at[f * parts + n])
            copy.start()
            copies.append(copy)
    for copy in copies:
        copy.wait()


def per_device(
    n_groups, n_tm, n_rows,
    features, spatial_weight, temporal_weight, head_weight, embed_weight, ada_scale, ada_shift, qkv_weight,
):
    frames, rows, columns, channels = features.shape
    depth, width = qkv_weight.shape
    pdim, wide_all = embed_weight.shape
    latent = head_weight.shape[1]
    split = n_groups == 2
    depth = depth // 2 if split else depth
    aligned = depth % LANES == 0
    quads = (2 if split else 1) * (2 if n_tm >= 4 else 1)
    later = max(n_tm.bit_length() - 3, 0)
    block_rows = pdim // (2 * quads)
    fold_shape = (2, quads, block_rows, width)
    part = embed_weight
    scale, shift = (v.reshape(wide_all // LANES, LANES) for v in (ada_scale, ada_shift))
    if not aligned:
        scale, shift = ada_scale[None], ada_shift[None]
        start = lax.axis_index("tm") * qkv_weight.shape[0]
        if split:
            start = start + lax.axis_index("groups") * depth
        scale, shift, part = (lax.dynamic_slice_in_dim(v, start, depth, axis=1) for v in (scale, shift, part))
    hbm = pl.BlockSpec(memory_space=pl.ANY)
    vmem = pl.BlockSpec(memory_space=pltpu.VMEM)
    tokens = columns // PATCH
    dma = pltpu.SemaphoreType.DMA
    block, fold, shift_row, gram = pl.pallas_call(
        functools.partial(encode, n_tm, n_rows, split, aligned),
        out_shape=(
            pltpu.VMEM((frames, n_rows, tokens, LANES), BF16),
            pltpu.VMEM(fold_shape, BF16),
            pltpu.VMEM((1, width), F32),
            pltpu.VMEM((3, pdim, pdim), BF16),
        ),
        in_specs=[hbm] * 9,
        out_specs=(vmem, vmem, vmem, vmem),
        scratch_shapes=[
            pltpu.VMEM(features.shape, BF16),
            pltpu.VMEM((frames, 2, columns, channels), BF16),
            pltpu.VMEM((frames, columns, (rows + 2) * 3 * channels), BF16),
            pltpu.VMEM((9 * channels, channels), BF16),
            pltpu.VMEM((3, channels, channels), BF16),
            pltpu.VMEM((latent, channels), BF16),
            pltpu.VMEM((pdim, wide_all), BF16),
            pltpu.VMEM((pdim, depth), BF16),
            pltpu.VMEM(scale.shape, BF16),
            pltpu.VMEM(shift.shape, BF16),
            pltpu.VMEM((2, wide_all // LANES, LANES), F32),
            pltpu.VMEM((2 * pdim, wide_all), BF16),
            pltpu.VMEM((depth, width), BF16),
            pltpu.VMEM((frames, rows * columns, channels), BF16),
            pltpu.VMEM((frames, rows * columns, channels), BF16),
            pltpu.VMEM((rows * columns, channels), BF16),
            pltpu.VMEM((frames, rows * columns, channels), F32),
            pltpu.VMEM((columns, LANES), F32),
            pltpu.VMEM((tokens, LANES), BF16),
            pltpu.VMEM(fold_shape, BF16),
            pltpu.VMEM(fold_shape[1:], BF16),
            pltpu.VMEM(fold_shape, F32),
            pltpu.VMEM(fold_shape[1:], BF16),
            pltpu.VMEM(fold_shape[1:], BF16),
            pltpu.VMEM((max(2 * later, 1), block_rows, width), BF16),
            pltpu.VMEM(fold_shape, BF16),
            pltpu.VMEM((2 + later, 1, width), F32),
            pltpu.VMEM((quads + later, 1, width), F32),
            pltpu.VMEM((frames, n_rows, tokens, LANES), BF16),
            pltpu.VMEM((PATCH, channels, LANES), BF16),
            dma((9 if aligned else 10,)),
            dma((2,)), dma((frames, 2)),
            dma((2,)), dma((2,)),
            dma((1,)), dma((1,)), dma((1,)), dma((1,)), dma((1,)),
            dma((4 + later,)), dma((4 + later,)),
            dma((2 + later,)), dma((2 + later,)),
            pltpu.SemaphoreType.REGULAR((max(n_rows - 1, 1),)),
            pltpu.SemaphoreType.REGULAR((1,)),
        ],
        compiler_params=pltpu.CompilerParams(
            collective_id=0, has_side_effects=True, vmem_limit_bytes=56 * 2**20
        ),
        name="encode",
    )(
        features,
        spatial_weight.reshape(9 * channels, channels),
        temporal_weight,
        head_weight.T,
        embed_weight,
        part,
        scale,
        shift,
        qkv_weight,
    )
    count = frames * n_rows * tokens
    return pl.pallas_call(
        project,
        out_shape=jax.ShapeDtypeStruct((count, width), F32),
        in_specs=[vmem] * 4,
        out_specs=hbm,
        scratch_shapes=[pltpu.VMEM((count, width), F32), dma((4 * frames,))],
        compiler_params=pltpu.CompilerParams(vmem_limit_bytes=32 * 2**20),
        name="project",
    )(block, fold.reshape(pdim, width), shift_row, gram)


def solution(mesh):
    return jax.shard_map(
        functools.partial(per_device, mesh.shape["groups"], mesh.shape["tm"], mesh.shape["rows"]),
        mesh=mesh,
        in_specs=(
            P(("groups", "tm"), "rows", None, None),
            P(),
            P(),
            P(),
            P(),
            P(),
            P(),
            P("tm", "rows"),
        ),
        out_specs=P(("groups", "tm"), "rows"),
        check_vma=False,
    )
```

```python
import functools

import jax
import jax.numpy as jnp
from jax import lax
from jax.experimental import pallas as pl
from jax.experimental.pallas import tpu as pltpu
from jax.sharding import PartitionSpec as P

MESH = pl.DeviceIdType.MESH
PATCH = 2
LANES = 128
EPS = 1e-06
F32 = jnp.float32
BF16 = jnp.bfloat16


def dot(a, b):
    return jnp.dot(a, b, preferred_element_type=F32)


def dot_t(a, b):
    return lax.dot_general(a, b, (((1,), (1,)), ((), ())), preferred_element_type=F32)


def norm_silu(values):
    scaled = values * lax.rsqrt(jnp.mean(values * values, axis=-1, keepdims=True) + EPS)
    half = 0.5 * scaled
    return half + half * jnp.tanh(half)


def encode(
    n_tm, n_rows, split, aligned,
    features, spatial_hbm, temporal_hbm, head_hbm, embed_hbm, part_hbm, scale_hbm, shift_hbm, qkv_hbm,
    block_out, fold_out, shift_out, gram_out,
    feat, halo, taps, spat_w, temp_w, head_w, embed, part, scale_v, shift_v, vectors, wide, qkv_w,
    mixed, side, bracket, partial, lat, ahead, part_b, core_in, keep, cross, quad_in, stage, fold, shifts, shifts_in, gathered, heads,
    load_sem, halo_send, halo_recv, mix_send, mix_recv,
    all_send, all_recv, ahead_send, ahead_recv, zero_send,
    fold_send, fold_recv, shift_send, shift_recv, relay, corner,
):
    group, tile, row = lax.axis_index("groups"), lax.axis_index("tm"), lax.axis_index("rows")
    frames, rows, columns, channels = features.shape
    depth, width = qkv_w.shape
    pdim, wide_all = embed.shape
    latent = head_w.shape[0]
    _, quads, block_rows, _ = fold.shape
    has_above, has_below = row > 0, row < n_rows - 1
    has_before, has_after = tile > 0, tile < n_tm - 1
    near = [({"rows": row - 1}, has_above), ({"rows": row + 1}, has_below)]
    count_rows = has_above.astype(jnp.int32) + has_below.astype(jnp.int32)
    count_tiles = has_before.astype(jnp.int32) + has_after.astype(jnp.int32)
    core = lax.rem(tile, 2)
    other_core = {"tm": tile + 1 - 2 * core}

    def flipped(bit):
        return tile + bit * (1 - 2 * lax.rem(tile // bit, 2))

    bits = [("tm", lax.rem(tile // 2, 2), flipped(2))] if n_tm >= 4 else []
    if split:
        bits.append(("groups", group, 1 - group))
    mine = sum((bit[1] * 2**n for n, bit in enumerate(bits)), 0)
    direct = []
    for mask in range(1, quads):
        chosen = [n for n in range(len(bits)) if mask >> n & 1]
        place = mine + sum(2**n * (1 - 2 * bits[n][1]) for n in chosen)
        direct.append(({bits[n][0]: bits[n][2] for n in chosen}, place))
    later = []
    step = 4
    while step < n_tm:
        later.append({"tm": flipped(step)})
        step *= 2
    partners = [other_core] + [device for device, _ in direct if len(device) == 1] + later

    def signal(sem, device):
        pl.semaphore_signal(sem, inc=1, device_id=device, device_id_type=MESH)

    barrier = pltpu.get_barrier_semaphore()
    for device in partners:
        signal(barrier, device)
    for device, there in near + [({"tm": tile - 1}, has_before), ({"tm": tile + 1}, has_after)]:

        @pl.when(there)
        def _():
            signal(barrier, device)

    def load(source, target, index):
        copy = pltpu.make_async_copy(source, target, load_sem.at[index])
        copy.start()
        return copy

    first = group * depth if split else 0
    load_feat = load(features, feat, 0)
    load_embed = load(embed_hbm, embed, 1)
    load_scale = load(scale_hbm, scale_v, 2)
    load_shift = load(shift_hbm, shift_v, 3)
    if not aligned:
        load_part = load(part_hbm, part, 9)
    load_qkv = load(qkv_hbm.at[pl.ds(pl.multiple_of(first, 16), depth)], qkv_w, 4)
    span = 3 * channels
    load_spat = [
        load(spatial_hbm.at[lines], spat_w.at[lines], index)
        for lines, index in ((pl.ds(span, 2 * span), 5), (pl.ds(0, span), 8))
    ]
    load_temp = load(temporal_hbm, temp_w, 6)
    load_head = load(head_hbm, head_w, 7)

    def remote(source, target, send, recv, device):
        return pltpu.make_async_remote_copy(
            src_ref=source, dst_ref=target, send_sem=send, recv_sem=recv,
            device_id=device, device_id_type=MESH,
        )

    def up_copy(f):
        return remote(
            features.at[f, 0], halo.at[f, 1], halo_send.at[0], halo_recv.at[f, 1], near[0][0]
        )

    def down_copy(f):
        return remote(
            features.at[f, rows - 1], halo.at[f, 0], halo_send.at[1], halo_recv.at[f, 0], near[1][0]
        )

    onward = remote(mixed.at[1], side.at[0], mix_send.at[1], mix_recv.at[0], {"tm": tile + 1})
    back = remote(bracket, side.at[1], mix_send.at[0], mix_recv.at[1], {"tm": tile - 1})

    order = (core, 1 - core)
    pl.semaphore_wait(barrier, len(partners) + count_rows + count_tiles)

    def send_rows(f):
        @pl.when(has_above)
        def _():
            up_copy(f).start()

        @pl.when(has_below)
        def _():
            down_copy(f).start()

    send_rows(order[0])

    phases = n_rows - 1
    done_phases = [0]

    def tell(phase):
        if phase < phases:
            for device, there in near:

                @pl.when(there)
                def _():
                    signal(relay.at[phase], device)

    def next_phase():
        phase = done_phases[0]
        if phase < phases:
            pl.semaphore_wait(relay.at[phase], count_rows)
            tell(phase + 1)
            done_phases[0] = phase + 1

    tell(0)
    if len(bits) == 2:
        signal(corner.at[0], {bits[1][0]: bits[1][2]})

    @pl.when(jnp.logical_not(has_above))
    def _():
        for f in range(frames):
            halo[f, 0] = jnp.zeros(halo.shape[2:], BF16)

    @pl.when(jnp.logical_not(has_below))
    def _():
        for f in range(frames):
            halo[f, 1] = jnp.zeros(halo.shape[2:], BF16)

    @pl.when(jnp.logical_not(has_before))
    def _():
        side[0] = jnp.zeros(side.shape[1:], BF16)

    column = lax.broadcasted_iota(jnp.int32, (columns, channels), 0)

    def spread_taps(values, place, frame):
        active = norm_silu(values.astype(F32))
        left = jnp.where(column == 0, 0.0, pltpu.roll(active, 1, 0))
        right = jnp.where(column == columns - 1, 0.0, pltpu.roll(active, columns - 1, 0))
        for k, shifted in enumerate((left, active, right)):
            taps[frame, :, pl.ds(place * span + k * channels, channels)] = shifted.astype(BF16)

    load_feat.wait()
    for f in range(frames):
        for r in range(rows):
            spread_taps(feat[f, r], r + 1, f)

    load_embed.wait()
    load_scale.wait()
    load_shift.wait()
    mean = jnp.mean(embed[...].astype(F32), axis=1, keepdims=True)
    if aligned:
        start = pl.multiple_of(tile * (wide_all // n_tm) + first, LANES)
        own = embed[:, pl.ds(start, depth)].astype(F32)
        vectors[0] = scale_v[...].astype(F32)
        vectors[1] = shift_v[...].astype(F32)
        at = start // LANES
        scale, shift = (
            jnp.concatenate([vectors[v, pl.ds(at + j, 1)] for j in range(depth // LANES)], axis=1)
            for v in range(2)
        )
    else:
        load_part.wait()
        own, scale, shift = part[...].astype(F32), scale_v[...].astype(F32), shift_v[...].astype(F32)
    scaled = (own - mean) * (1.0 + scale)
    upper = scaled.astype(BF16)
    lower = (scaled - upper.astype(F32)).astype(BF16)
    rows16 = lax.broadcasted_iota(jnp.int32, (16, depth), 0)
    shift16 = jnp.where(rows16 == 0, jnp.broadcast_to(shift, (16, depth)), 0.0).astype(BF16)
    lhs = jnp.concatenate([upper, lower, shift16], axis=0)
    load_qkv.wait()
    chunk = width // 3
    for n in range(3):
        cols = pl.ds(n * chunk, chunk)
        terms = dot(lhs, qkv_w[:, cols])
        shifts[0, :, cols] = terms[2 * pdim : 2 * pdim + 1]
        terms = terms[:pdim] + terms[pdim : 2 * pdim]
        for c in range(2):
            for b in range(quads):
                low = (c * quads + b) * block_rows
                piece = terms[low : low + block_rows]
                keep[c, b, :, cols] = piece
                part_b[c, b, :, cols] = piece.astype(BF16)

    core_copies = [
        remote(part_b.at[1 - core], core_in, fold_send.at[0], fold_recv.at[0], other_core),
        remote(shifts.at[0], shifts_in.at[0], shift_send.at[0], shift_recv.at[0], other_core),
    ]
    for copy in core_copies:
        copy.start()
    send_rows(order[1])

    inner = taps[:, :, span : 3 * span].reshape(frames * columns, 2 * span)
    direct_copies = []
    for r in range(rows):
        load_spat[r].wait()
        total = dot(inner, spat_w[(1 - r) * span : (3 - r) * span])
        for f in range(frames):
            partial[f, pl.ds(r * columns, columns)] = total[f * columns : (f + 1) * columns]
        if r == 0:
            for copy in core_copies:
                copy.wait()
            shifts[1] = shifts[0] + shifts_in[0]
            for b in range(quads):
                cross[b] = (keep[core, b] + core_in[b].astype(F32)).astype(BF16)
            for m, (device, place) in enumerate(direct, 1):
                direct_copies += [
                    remote(cross.at[place], quad_in.at[m], fold_send.at[1], fold_recv.at[1], device),
                    remote(shifts.at[1], shifts_in.at[m], shift_send.at[1], shift_recv.at[1], device),
                ]
            if len(bits) == 2:
                pl.semaphore_wait(corner.at[0], 1)
            for copy in direct_copies:
                copy.start()
    next_phase()

    def end_direct():
        total = keep[core, mine] + core_in[mine].astype(F32)
        shift_total = shifts[1]
        if direct:
            device = direct[0][0]
            for copy in (
                remote(quad_in.at[1:], quad_in.at[1:], fold_send.at[1], fold_recv.at[1], device),
                remote(
                    shifts_in.at[1:quads], shifts_in.at[1:quads], shift_send.at[1], shift_recv.at[1], device
                ),
            ):
                copy.wait()
        for m in range(1, quads):
            total = total + quad_in[m].astype(F32)
            shift_total = shift_total + shifts_in[m]
        for n, device in enumerate(later):
            stage[2 * n] = total.astype(BF16)
            shifts[2 + n] = shift_total
            pair_copies = [
                remote(
                    stage.at[2 * n], stage.at[2 * n + 1],
                    fold_send.at[2 + n], fold_recv.at[2 + n], device,
                ),
                remote(
                    shifts.at[2 + n], shifts_in.at[quads + n],
                    shift_send.at[2 + n], shift_recv.at[2 + n], device,
                ),
            ]
            for copy in pair_copies:
                copy.start()
            for copy in pair_copies:
                copy.wait()
            total = total + stage[2 * n + 1].astype(F32)
            shift_total = shift_total + shifts_in[quads + n]
        fold[core, mine] = total.astype(BF16)
        shift_out[...] = shift_total
        for copy in share_copies:
            copy.start()

    base = 2 + len(later)
    share_copies = [
        remote(fold.at[core, mine], fold.at[core, mine], fold_send.at[base], fold_recv.at[base], device)
        for device, _ in direct
    ]

    load_head.wait()

    def place_heads():
        lane = lax.broadcasted_iota(jnp.int32, (latent, LANES), 1)
        latent_lane = lax.broadcasted_iota(jnp.int32, (latent, LANES), 0)
        pair = PATCH * latent
        for a in range(PATCH):
            low = a * pair
            pick = (lane >= low) & (lane < low + pair) & (lax.rem(lane, latent) == latent_lane)
            spread_head = lax.dot_general(
                head_w[...], jnp.where(pick, 1.0, 0.0).astype(BF16), (((0,), (0,)), ((), ())),
                preferred_element_type=F32,
            )
            heads[a] = spread_head.astype(BF16)

    load_temp.wait()

    def finish_frame(f):
        @pl.when(has_above)
        def _():
            down_copy(f).wait_recv()

        @pl.when(has_below)
        def _():
            up_copy(f).wait_recv()

        spread_taps(halo[f, 0], 0, f)
        spread_taps(halo[f, 1], rows + 1, f)
        totals = []
        for r, (place, weights) in enumerate(
            ((0, spat_w[0:span]), (3 * span, spat_w[2 * span : 3 * span]))
        ):
            lines = pl.ds(r * columns, columns)
            totals.append(partial[f, lines] + dot(taps[f, :, pl.ds(place, span)], weights))
        mixed[f] = norm_silu(jnp.concatenate(totals, axis=0)).astype(BF16)

        @pl.when(jnp.logical_and(f == 1, has_after))
        def _():
            onward.start()

        @pl.when(f == 0)
        def _():
            residual = jnp.concatenate([feat[0, r].astype(F32) for r in range(rows)], axis=0)
            bracket[...] = (dot(mixed[0], temp_w[2]) + residual).astype(BF16)

            @pl.when(has_before)
            def _():
                back.start()

    @pl.when(core == 0)
    def _():
        place_heads()

    early = 2 * row < n_rows
    soon = jnp.logical_and(early, lax.rem(tile // 2, 2) == 1)
    finish_frame(order[0])
    next_phase()

    @pl.when(soon)
    def _():
        end_direct()

    finish_frame(order[1])

    @pl.when(core == 1)
    def _():
        place_heads()

    @pl.when(jnp.logical_and(early, jnp.logical_not(soon)))
    def _():
        end_direct()

    tokens = columns // PATCH
    out_lane = lax.broadcasted_iota(jnp.int32, (tokens, LANES), 1)
    even_lane = lax.rem(out_lane // latent, PATCH) == 0

    def patches_of(total):
        active = norm_silu(total).astype(BF16)
        lat[...] = dot(active[:columns], heads[0]) + dot(active[columns:], heads[1])
        even = lat[pl.ds(0, tokens, stride=PATCH), :]
        odd = lat[pl.ds(1, tokens, stride=PATCH), :]
        return jnp.where(even_lane, even, odd).astype(BF16)

    def away(d):
        return lax.rem(row + d, n_rows)

    sends = [
        remote(
            gathered.at[1, row], gathered.at[1, row], all_send.at[0], all_recv.at[0], {"rows": away(d)}
        )
        for d in range(1, n_rows)
    ]
    ahead_sends = [
        remote(
            ahead, gathered.at[0, row], ahead_send.at[0], ahead_recv.at[0],
            {"tm": tile + 1, "rows": away(d)},
        )
        for d in range(n_rows)
    ]
    zero_sends = [
        remote(
            gathered.at[0, row], gathered.at[0, row], zero_send.at[0], ahead_recv.at[0], {"rows": away(d)}
        )
        for d in range(1, n_rows)
    ]

    is_first = tile == 0
    last_first = jnp.logical_or(is_first, core == 1)

    def of_own(tap):
        own_frames = jnp.concatenate([mixed[0], mixed[1]], axis=1)
        return dot(own_frames, temp_w[tap : tap + 2].reshape(2 * channels, channels))

    @pl.when(last_first)
    def _():
        partial[1] = of_own(1)

    @pl.when(jnp.logical_not(last_first))
    def _():
        partial[0] = of_own(0)

    @pl.when(is_first)
    def _():
        gathered[0, row] = patches_of(bracket[...].astype(F32))

    while done_phases[0] < phases:
        next_phase()

    @pl.when(is_first)
    def _():
        for copy in zero_sends:
            copy.start()

    def last_frame():
        @pl.when(has_before)
        def _():
            onward.wait_recv()

        residual = jnp.concatenate([feat[1, r].astype(F32) for r in range(rows)], axis=0)
        gathered[1, row] = patches_of(partial[1] + dot(side[0], temp_w[0]) + residual)
        for copy in sends:
            copy.start()

    late = jnp.logical_not(early)

    @pl.when(last_first)
    def _():
        last_frame()

    @pl.when(jnp.logical_and(last_first, late))
    def _():
        end_direct()

    @pl.when(has_after)
    def _():
        @pl.when(last_first)
        def _():
            partial[0] = of_own(0)

        back.wait_recv()
        ahead[...] = patches_of(partial[0] + side[1].astype(F32))
        for copy in ahead_sends:
            copy.start()

    @pl.when(jnp.logical_and(jnp.logical_not(last_first), late))
    def _():
        end_direct()

    @pl.when(jnp.logical_not(last_first))
    def _():
        partial[1] = of_own(1)
        last_frame()

    if direct:
        others = fold.at[core, 0 : quads - 1]
        remote(others, others, fold_send.at[base], fold_recv.at[base], direct[0][0]).wait()
    base += 1
    widen = remote(fold.at[core], fold.at[core], fold_send.at[base], fold_recv.at[base], other_core)
    widen.start()

    centred = embed[...].astype(F32) - mean
    high = centred.astype(BF16)
    wide[0:pdim] = high
    wide[pdim:] = (centred - high.astype(F32)).astype(BF16)
    products = dot_t(wide[...], wide[...])
    gram = (
        products[:pdim, :pdim] + products[:pdim, pdim:]
        + products[pdim:, :pdim] + products[pdim:, pdim:]
    ) * (1.0 / wide_all)
    for i in range(3):
        piece = gram.astype(BF16)
        gram_out[i] = piece
        gram = gram - piece.astype(F32)

    @pl.when(has_above)
    def _():
        edge = features.at[:, 0]
        remote(edge, halo.at[:, 1], halo_send.at[0], halo_recv.at[0, 1], near[0][0]).wait_send()

    @pl.when(has_below)
    def _():
        edge = features.at[:, rows - 1]
        remote(edge, halo.at[:, 0], halo_send.at[1], halo_recv.at[0, 0], near[1][0]).wait_send()

    @pl.when(has_before)
    def _():
        back.wait_send()

    def all_of(frame, count, send, recv):
        several = gathered.at[frame, 0:count]
        return remote(several, several, send.at[0], recv.at[0], other_core)

    @pl.when(has_after)
    def _():
        onward.wait_send()
        all_of(0, n_rows, ahead_send, ahead_recv).wait_send()

    if n_rows > 1:

        @pl.when(is_first)
        def _():
            all_of(0, n_rows - 1, zero_send, ahead_recv).wait_send()

    widen.wait()
    fold_out[...] = fold[...]
    if n_rows > 1:
        all_of(1, n_rows - 1, all_send, all_recv).wait()

        @pl.when(is_first)
        def _():
            all_of(0, n_rows - 1, zero_send, ahead_recv).wait_recv()

    @pl.when(has_before)
    def _():
        all_of(0, n_rows, ahead_send, ahead_recv).wait_recv()

    block_out[...] = gathered[...]


def project(block, fold, shift, gram, out, held, sems):
    pdim, width = fold.shape
    frames, n_rows, tokens, _ = block.shape
    parts = 4
    lines = n_rows * tokens // parts
    copies = []
    for f in range(frames):
        patches = block[f].reshape(n_rows * tokens, LANES)[:, :pdim]
        for n in range(parts):
            own = patches[n * lines : (n + 1) * lines]
            moved = dot(own, gram[0]) + dot(own, gram[1]) + dot(own, gram[2])
            spread = jnp.maximum(jnp.sum(moved * own.astype(F32), axis=-1, keepdims=True), 0.0)
            here = pl.ds((f * parts + n) * lines, lines)
            held[here] = dot(own, fold[...]) * lax.rsqrt(spread + EPS) + shift[...]
            copy = pltpu.make_async_copy(held.at[here], out.at[here], sems.at[f * parts + n])
            copy.start()
            copies.append(copy)
    for copy in copies:
        copy.wait()


def per_device(
    n_groups, n_tm, n_rows,
    features, spatial_weight, temporal_weight, head_weight, embed_weight, ada_scale, ada_shift, qkv_weight,
):
    frames, rows, columns, channels = features.shape
    depth, width = qkv_weight.shape
    pdim, wide_all = embed_weight.shape
    latent = head_weight.shape[1]
    split = n_groups == 2
    depth = depth // 2 if split else depth
    aligned = depth % LANES == 0
    quads = (2 if split else 1) * (2 if n_tm >= 4 else 1)
    later = max(n_tm.bit_length() - 3, 0)
    block_rows = pdim // (2 * quads)
    fold_shape = (2, quads, block_rows, width)
    part = embed_weight
    scale, shift = (v.reshape(wide_all // LANES, LANES) for v in (ada_scale, ada_shift))
    if not aligned:
        scale, shift = ada_scale[None], ada_shift[None]
        start = lax.axis_index("tm") * qkv_weight.shape[0]
        if split:
            start = start + lax.axis_index("groups") * depth
        scale, shift, part = (lax.dynamic_slice_in_dim(v, start, depth, axis=1) for v in (scale, shift, part))
    hbm = pl.BlockSpec(memory_space=pl.ANY)
    vmem = pl.BlockSpec(memory_space=pltpu.VMEM)
    tokens = columns // PATCH
    dma = pltpu.SemaphoreType.DMA
    block, fold, shift_row, gram = pl.pallas_call(
        functools.partial(encode, n_tm, n_rows, split, aligned),
        out_shape=(
            pltpu.VMEM((frames, n_rows, tokens, LANES), BF16),
            pltpu.VMEM(fold_shape, BF16),
            pltpu.VMEM((1, width), F32),
            pltpu.VMEM((3, pdim, pdim), BF16),
        ),
        in_specs=[hbm] * 9,
        out_specs=(vmem, vmem, vmem, vmem),
        scratch_shapes=[
            pltpu.VMEM(features.shape, BF16),
            pltpu.VMEM((frames, 2, columns, channels), BF16),
            pltpu.VMEM((frames, columns, (rows + 2) * 3 * channels), BF16),
            pltpu.VMEM((9 * channels, channels), BF16),
            pltpu.VMEM((3, channels, channels), BF16),
            pltpu.VMEM((latent, channels), BF16),
            pltpu.VMEM((pdim, wide_all), BF16),
            pltpu.VMEM((pdim, depth), BF16),
            pltpu.VMEM(scale.shape, BF16),
            pltpu.VMEM(shift.shape, BF16),
            pltpu.VMEM((2, wide_all // LANES, LANES), F32),
            pltpu.VMEM((2 * pdim, wide_all), BF16),
            pltpu.VMEM((depth, width), BF16),
            pltpu.VMEM((frames, rows * columns, channels), BF16),
            pltpu.VMEM((frames, rows * columns, channels), BF16),
            pltpu.VMEM((rows * columns, channels), BF16),
            pltpu.VMEM((frames, rows * columns, channels), F32),
            pltpu.VMEM((columns, LANES), F32),
            pltpu.VMEM((tokens, LANES), BF16),
            pltpu.VMEM(fold_shape, BF16),
            pltpu.VMEM(fold_shape[1:], BF16),
            pltpu.VMEM(fold_shape, F32),
            pltpu.VMEM(fold_shape[1:], BF16),
            pltpu.VMEM(fold_shape[1:], BF16),
            pltpu.VMEM((max(2 * later, 1), block_rows, width), BF16),
            pltpu.VMEM(fold_shape, BF16),
            pltpu.VMEM((2 + later, 1, width), F32),
            pltpu.VMEM((quads + later, 1, width), F32),
            pltpu.VMEM((frames, n_rows, tokens, LANES), BF16),
            pltpu.VMEM((PATCH, channels, LANES), BF16),
            dma((9 if aligned else 10,)),
            dma((2,)), dma((frames, 2)),
            dma((2,)), dma((2,)),
            dma((1,)), dma((1,)), dma((1,)), dma((1,)), dma((1,)),
            dma((4 + later,)), dma((4 + later,)),
            dma((2 + later,)), dma((2 + later,)),
            pltpu.SemaphoreType.REGULAR((max(n_rows - 1, 1),)),
            pltpu.SemaphoreType.REGULAR((1,)),
        ],
        compiler_params=pltpu.CompilerParams(
            collective_id=0, has_side_effects=True, vmem_limit_bytes=56 * 2**20
        ),
        name="encode",
    )(
        features,
        spatial_weight.reshape(9 * channels, channels),
        temporal_weight,
        head_weight.T,
        embed_weight,
        part,
        scale,
        shift,
        qkv_weight,
    )
    count = frames * n_rows * tokens
    return pl.pallas_call(
        project,
        out_shape=jax.ShapeDtypeStruct((count, width), F32),
        in_specs=[vmem] * 4,
        out_specs=hbm,
        scratch_shapes=[pltpu.VMEM((count, width), F32), dma((4 * frames,))],
        compiler_params=pltpu.CompilerParams(vmem_limit_bytes=32 * 2**20),
        name="project",
    )(block, fold.reshape(pdim, width), shift_row, gram)


def solution(mesh):
    return jax.shard_map(
        functools.partial(per_device, mesh.shape["groups"], mesh.shape["tm"], mesh.shape["rows"]),
        mesh=mesh,
        in_specs=(
            P(("groups", "tm"), "rows", None, None),
            P(),
            P(),
            P(),
            P(),
            P(),
            P(),
            P("tm", "rows"),
        ),
        out_specs=P(("groups", "tm"), "rows"),
        check_vma=False,
    )
```

```python
import functools

import jax
import jax.numpy as jnp
from jax import lax
from jax.experimental import pallas as pl
from jax.experimental.pallas import tpu as pltpu
from jax.sharding import PartitionSpec as P

MESH = pl.DeviceIdType.MESH
PATCH = 2
LANES = 128
EPS = 1e-06
F32 = jnp.float32
BF16 = jnp.bfloat16


def dot(a, b):
    return jnp.dot(a, b, preferred_element_type=F32)


def dot_t(a, b):
    return lax.dot_general(a, b, (((1,), (1,)), ((), ())), preferred_element_type=F32)


def norm_silu(values):
    scaled = values * lax.rsqrt(jnp.mean(values * values, axis=-1, keepdims=True) + EPS)
    half = 0.5 * scaled
    return half + half * jnp.tanh(half)


def encode(
    n_tm, n_rows, split, aligned,
    features, spatial_hbm, temporal_hbm, head_hbm, embed_hbm, part_hbm, scale_hbm, shift_hbm, qkv_hbm,
    block_out, fold_out, shift_out, gram_out,
    feat, halo, taps, spat_w, temp_w, head_w, embed, part, scale_v, shift_v, vectors, wide, qkv_w,
    mixed, side, bracket, partial, lat, ahead, part_b, core_in, keep, cross, quad_in, stage, fold, shifts, shifts_in, gathered, heads,
    load_sem, halo_send, halo_recv, mix_send, mix_recv,
    all_send, all_recv, ahead_send, ahead_recv, zero_send,
    fold_send, fold_recv, shift_send, shift_recv, relay, corner,
):
    group, tile, row = lax.axis_index("groups"), lax.axis_index("tm"), lax.axis_index("rows")
    frames, rows, columns, channels = features.shape
    depth, width = qkv_w.shape
    pdim, wide_all = embed.shape
    latent = head_w.shape[0]
    _, quads, block_rows, _ = fold.shape
    has_above, has_below = row > 0, row < n_rows - 1
    has_before, has_after = tile > 0, tile < n_tm - 1
    near = [({"rows": row - 1}, has_above), ({"rows": row + 1}, has_below)]
    count_rows = has_above.astype(jnp.int32) + has_below.astype(jnp.int32)
    count_tiles = has_before.astype(jnp.int32) + has_after.astype(jnp.int32)
    core = lax.rem(tile, 2)
    other_core = {"tm": tile + 1 - 2 * core}

    def flipped(bit):
        return tile + bit * (1 - 2 * lax.rem(tile // bit, 2))

    bits = [("tm", lax.rem(tile // 2, 2), flipped(2))] if n_tm >= 4 else []
    if split:
        bits.append(("groups", group, 1 - group))
    mine = sum((bit[1] * 2**n for n, bit in enumerate(bits)), 0)
    direct = []
    for mask in range(1, quads):
        chosen = [n for n in range(len(bits)) if mask >> n & 1]
        place = mine + sum(2**n * (1 - 2 * bits[n][1]) for n in chosen)
        direct.append(({bits[n][0]: bits[n][2] for n in chosen}, place))
    later = []
    step = 4
    while step < n_tm:
        later.append({"tm": flipped(step)})
        step *= 2
    partners = [other_core] + [device for device, _ in direct if len(device) == 1] + later

    def signal(sem, device):
        pl.semaphore_signal(sem, inc=1, device_id=device, device_id_type=MESH)

    barrier = pltpu.get_barrier_semaphore()
    for device in partners:
        signal(barrier, device)
    for device, there in near + [({"tm": tile - 1}, has_before), ({"tm": tile + 1}, has_after)]:

        @pl.when(there)
        def _():
            signal(barrier, device)

    def load(source, target, index):
        copy = pltpu.make_async_copy(source, target, load_sem.at[index])
        copy.start()
        return copy

    first = group * depth if split else 0
    load_feat = load(features, feat, 0)
    load_embed = load(embed_hbm, embed, 1)
    load_scale = load(scale_hbm, scale_v, 2)
    load_shift = load(shift_hbm, shift_v, 3)
    if not aligned:
        load_part = load(part_hbm, part, 9)
    load_qkv = load(qkv_hbm.at[pl.ds(pl.multiple_of(first, 16), depth)], qkv_w, 4)
    span = 3 * channels
    load_spat = [
        load(spatial_hbm.at[lines], spat_w.at[lines], index)
        for lines, index in ((pl.ds(span, 2 * span), 5), (pl.ds(0, span), 8))
    ]
    load_temp = load(temporal_hbm, temp_w, 6)
    load_head = load(head_hbm, head_w, 7)

    def remote(source, target, send, recv, device):
        return pltpu.make_async_remote_copy(
            src_ref=source, dst_ref=target, send_sem=send, recv_sem=recv,
            device_id=device, device_id_type=MESH,
        )

    def up_copy(f):
        return remote(
            features.at[f, 0], halo.at[f, 1], halo_send.at[0], halo_recv.at[f, 1], near[0][0]
        )

    def down_copy(f):
        return remote(
            features.at[f, rows - 1], halo.at[f, 0], halo_send.at[1], halo_recv.at[f, 0], near[1][0]
        )

    onward = remote(mixed.at[1], side.at[0], mix_send.at[1], mix_recv.at[0], {"tm": tile + 1})
    back = remote(bracket, side.at[1], mix_send.at[0], mix_recv.at[1], {"tm": tile - 1})

    order = (core, 1 - core)
    pl.semaphore_wait(barrier, len(partners) + count_rows + count_tiles)

    def send_rows(f):
        @pl.when(has_above)
        def _():
            up_copy(f).start()

        @pl.when(has_below)
        def _():
            down_copy(f).start()

    send_rows(order[0])

    phases = n_rows - 1
    done_phases = [0]

    def tell(phase):
        if phase < phases:
            for device, there in near:

                @pl.when(there)
                def _():
                    signal(relay.at[phase], device)

    def next_phase():
        phase = done_phases[0]
        if phase < phases:
            pl.semaphore_wait(relay.at[phase], count_rows)
            tell(phase + 1)
            done_phases[0] = phase + 1

    tell(0)
    if len(bits) == 2:
        signal(corner.at[0], {bits[1][0]: bits[1][2]})

    @pl.when(jnp.logical_not(has_above))
    def _():
        for f in range(frames):
            halo[f, 0] = jnp.zeros(halo.shape[2:], BF16)

    @pl.when(jnp.logical_not(has_below))
    def _():
        for f in range(frames):
            halo[f, 1] = jnp.zeros(halo.shape[2:], BF16)

    @pl.when(jnp.logical_not(has_before))
    def _():
        side[0] = jnp.zeros(side.shape[1:], BF16)

    column = lax.broadcasted_iota(jnp.int32, (columns, channels), 0)

    def spread_taps(values, place, frame):
        active = norm_silu(values.astype(F32))
        left = jnp.where(column == 0, 0.0, pltpu.roll(active, 1, 0))
        right = jnp.where(column == columns - 1, 0.0, pltpu.roll(active, columns - 1, 0))
        for k, shifted in enumerate((left, active, right)):
            taps[frame, :, pl.ds(place * span + k * channels, channels)] = shifted.astype(BF16)

    load_feat.wait()
    for f in range(frames):
        for r in range(rows):
            spread_taps(feat[f, r], r + 1, f)

    load_embed.wait()
    load_scale.wait()
    load_shift.wait()
    mean = jnp.mean(embed[...].astype(F32), axis=1, keepdims=True)
    if aligned:
        start = pl.multiple_of(tile * (wide_all // n_tm) + first, LANES)
        own = embed[:, pl.ds(start, depth)].astype(F32)
        vectors[0] = scale_v[...].astype(F32)
        vectors[1] = shift_v[...].astype(F32)
        at = start // LANES
        scale, shift = (
            jnp.concatenate([vectors[v, pl.ds(at + j, 1)] for j in range(depth // LANES)], axis=1)
            for v in range(2)
        )
    else:
        load_part.wait()
        own, scale, shift = part[...].astype(F32), scale_v[...].astype(F32), shift_v[...].astype(F32)
    scaled = (own - mean) * (1.0 + scale)
    upper = scaled.astype(BF16)
    lower = (scaled - upper.astype(F32)).astype(BF16)
    rows16 = lax.broadcasted_iota(jnp.int32, (16, depth), 0)
    shift16 = jnp.where(rows16 == 0, jnp.broadcast_to(shift, (16, depth)), 0.0).astype(BF16)
    lhs = jnp.concatenate([upper, lower, shift16], axis=0)
    load_qkv.wait()
    chunk = width // 3
    for n in range(3):
        cols = pl.ds(n * chunk, chunk)
        terms = dot(lhs, qkv_w[:, cols])
        shifts[0, :, cols] = terms[2 * pdim : 2 * pdim + 1]
        terms = terms[:pdim] + terms[pdim : 2 * pdim]
        for c in range(2):
            for b in range(quads):
                low = (c * quads + b) * block_rows
                piece = terms[low : low + block_rows]
                keep[c, b, :, cols] = piece
                part_b[c, b, :, cols] = piece.astype(BF16)

    core_copies = [
        remote(part_b.at[1 - core], core_in, fold_send.at[0], fold_recv.at[0], other_core),
        remote(shifts.at[0], shifts_in.at[0], shift_send.at[0], shift_recv.at[0], other_core),
    ]
    for copy in core_copies:
        copy.start()
    send_rows(order[1])

    inner = taps[:, :, span : 3 * span].reshape(frames * columns, 2 * span)
    direct_copies = []
    for r in range(rows):
        load_spat[r].wait()
        total = dot(inner, spat_w[(1 - r) * span : (3 - r) * span])
        for f in range(frames):
            partial[f, pl.ds(r * columns, columns)] = total[f * columns : (f + 1) * columns]
        if r == 0:
            for copy in core_copies:
                copy.wait()
            shifts[1] = shifts[0] + shifts_in[0]
            for b in range(quads):
                cross[b] = (keep[core, b] + core_in[b].astype(F32)).astype(BF16)
            for m, (device, place) in enumerate(direct, 1):
                direct_copies += [
                    remote(cross.at[place], quad_in.at[m], fold_send.at[1], fold_recv.at[1], device),
                    remote(shifts.at[1], shifts_in.at[m], shift_send.at[1], shift_recv.at[1], device),
                ]
            if len(bits) == 2:
                pl.semaphore_wait(corner.at[0], 1)
            for copy in direct_copies:
                copy.start()
    next_phase()

    def end_direct():
        total = keep[core, mine] + core_in[mine].astype(F32)
        shift_total = shifts[1]
        if direct:
            device = direct[0][0]
            for copy in (
                remote(quad_in.at[1:], quad_in.at[1:], fold_send.at[1], fold_recv.at[1], device),
                remote(
                    shifts_in.at[1:quads], shifts_in.at[1:quads], shift_send.at[1], shift_recv.at[1], device
                ),
            ):
                copy.wait()
        for m in range(1, quads):
            total = total + quad_in[m].astype(F32)
            shift_total = shift_total + shifts_in[m]
        for n, device in enumerate(later):
            stage[2 * n] = total.astype(BF16)
            shifts[2 + n] = shift_total
            pair_copies = [
                remote(
                    stage.at[2 * n], stage.at[2 * n + 1],
                    fold_send.at[2 + n], fold_recv.at[2 + n], device,
                ),
                remote(
                    shifts.at[2 + n], shifts_in.at[quads + n],
                    shift_send.at[2 + n], shift_recv.at[2 + n], device,
                ),
            ]
            for copy in pair_copies:
                copy.start()
            for copy in pair_copies:
                copy.wait()
            total = total + stage[2 * n + 1].astype(F32)
            shift_total = shift_total + shifts_in[quads + n]
        fold[core, mine] = total.astype(BF16)
        shift_out[...] = shift_total
        for copy in share_copies:
            copy.start()

    base = 2 + len(later)
    share_copies = [
        remote(fold.at[core, mine], fold.at[core, mine], fold_send.at[base], fold_recv.at[base], device)
        for device, _ in direct
    ]

    load_head.wait()

    def place_heads():
        lane = lax.broadcasted_iota(jnp.int32, (latent, LANES), 1)
        latent_lane = lax.broadcasted_iota(jnp.int32, (latent, LANES), 0)
        pair = PATCH * latent
        for a in range(PATCH):
            low = a * pair
            pick = (lane >= low) & (lane < low + pair) & (lax.rem(lane, latent) == latent_lane)
            spread_head = lax.dot_general(
                head_w[...], jnp.where(pick, 1.0, 0.0).astype(BF16), (((0,), (0,)), ((), ())),
                preferred_element_type=F32,
            )
            heads[a] = spread_head.astype(BF16)

    load_temp.wait()

    def finish_frame(f):
        @pl.when(has_above)
        def _():
            down_copy(f).wait_recv()

        @pl.when(has_below)
        def _():
            up_copy(f).wait_recv()

        spread_taps(halo[f, 0], 0, f)
        spread_taps(halo[f, 1], rows + 1, f)
        totals = []
        for r, (place, weights) in enumerate(
            ((0, spat_w[0:span]), (3 * span, spat_w[2 * span : 3 * span]))
        ):
            lines = pl.ds(r * columns, columns)
            totals.append(partial[f, lines] + dot(taps[f, :, pl.ds(place, span)], weights))
        mixed[f] = norm_silu(jnp.concatenate(totals, axis=0)).astype(BF16)

        @pl.when(jnp.logical_and(f == 1, has_after))
        def _():
            onward.start()

        @pl.when(f == 0)
        def _():
            residual = jnp.concatenate([feat[0, r].astype(F32) for r in range(rows)], axis=0)
            bracket[...] = (dot(mixed[0], temp_w[2]) + residual).astype(BF16)

            @pl.when(has_before)
            def _():
                back.start()

    @pl.when(core == 0)
    def _():
        place_heads()

    early = 2 * row < n_rows
    soon = jnp.logical_and(early, lax.rem(tile // 2, 2) == 1)
    is_first = tile == 0
    tokens = columns // PATCH
    out_lane = lax.broadcasted_iota(jnp.int32, (tokens, LANES), 1)
    even_lane = lax.rem(out_lane // latent, PATCH) == 0

    def patches_of(total):
        active = norm_silu(total).astype(BF16)
        lat[...] = dot(active[:columns], heads[0]) + dot(active[columns:], heads[1])
        even = lat[pl.ds(0, tokens, stride=PATCH), :]
        odd = lat[pl.ds(1, tokens, stride=PATCH), :]
        return jnp.where(even_lane, even, odd).astype(BF16)

    finish_frame(order[0])

    @pl.when(is_first)
    def _():
        gathered[0, row] = patches_of(bracket[...].astype(F32))

    next_phase()

    @pl.when(soon)
    def _():
        end_direct()

    finish_frame(order[1])

    @pl.when(core == 1)
    def _():
        place_heads()

    @pl.when(jnp.logical_and(early, jnp.logical_not(soon)))
    def _():
        end_direct()

    def away(d):
        return lax.rem(row + d, n_rows)

    sends = [
        remote(
            gathered.at[1, row], gathered.at[1, row], all_send.at[0], all_recv.at[0], {"rows": away(d)}
        )
        for d in range(1, n_rows)
    ]
    ahead_sends = [
        remote(
            ahead, gathered.at[0, row], ahead_send.at[0], ahead_recv.at[0],
            {"tm": tile + 1, "rows": away(d)},
        )
        for d in range(n_rows)
    ]
    zero_sends = [
        remote(
            gathered.at[0, row], gathered.at[0, row], zero_send.at[0], ahead_recv.at[0], {"rows": away(d)}
        )
        for d in range(1, n_rows)
    ]

    last_first = jnp.logical_or(is_first, core == 1)

    def of_own(tap):
        own_frames = jnp.concatenate([mixed[0], mixed[1]], axis=1)
        return dot(own_frames, temp_w[tap : tap + 2].reshape(2 * channels, channels))

    @pl.when(last_first)
    def _():
        partial[1] = of_own(1)

    @pl.when(jnp.logical_not(last_first))
    def _():
        partial[0] = of_own(0)

    while done_phases[0] < phases:
        next_phase()

    @pl.when(is_first)
    def _():
        for copy in zero_sends:
            copy.start()

    def last_frame():
        @pl.when(has_before)
        def _():
            onward.wait_recv()

        residual = jnp.concatenate([feat[1, r].astype(F32) for r in range(rows)], axis=0)
        gathered[1, row] = patches_of(partial[1] + dot(side[0], temp_w[0]) + residual)
        for copy in sends:
            copy.start()

    late = jnp.logical_not(early)

    @pl.when(last_first)
    def _():
        last_frame()

    @pl.when(jnp.logical_and(last_first, late))
    def _():
        end_direct()

    @pl.when(has_after)
    def _():
        @pl.when(last_first)
        def _():
            partial[0] = of_own(0)

        back.wait_recv()
        ahead[...] = patches_of(partial[0] + side[1].astype(F32))
        for copy in ahead_sends:
            copy.start()

    @pl.when(jnp.logical_and(jnp.logical_not(last_first), late))
    def _():
        end_direct()

    @pl.when(jnp.logical_not(last_first))
    def _():
        partial[1] = of_own(1)
        last_frame()

    if direct:
        others = fold.at[core, 0 : quads - 1]
        remote(others, others, fold_send.at[base], fold_recv.at[base], direct[0][0]).wait()
    base += 1
    widen = remote(fold.at[core], fold.at[core], fold_send.at[base], fold_recv.at[base], other_core)
    widen.start()

    centred = embed[...].astype(F32) - mean
    high = centred.astype(BF16)
    wide[0:pdim] = high
    wide[pdim:] = (centred - high.astype(F32)).astype(BF16)
    products = dot_t(wide[...], wide[...])
    gram = (
        products[:pdim, :pdim] + products[:pdim, pdim:]
        + products[pdim:, :pdim] + products[pdim:, pdim:]
    ) * (1.0 / wide_all)
    for i in range(3):
        piece = gram.astype(BF16)
        gram_out[i] = piece
        gram = gram - piece.astype(F32)

    @pl.when(has_above)
    def _():
        edge = features.at[:, 0]
        remote(edge, halo.at[:, 1], halo_send.at[0], halo_recv.at[0, 1], near[0][0]).wait_send()

    @pl.when(has_below)
    def _():
        edge = features.at[:, rows - 1]
        remote(edge, halo.at[:, 0], halo_send.at[1], halo_recv.at[0, 0], near[1][0]).wait_send()

    @pl.when(has_before)
    def _():
        back.wait_send()

    def all_of(frame, count, send, recv):
        several = gathered.at[frame, 0:count]
        return remote(several, several, send.at[0], recv.at[0], other_core)

    @pl.when(has_after)
    def _():
        onward.wait_send()
        all_of(0, n_rows, ahead_send, ahead_recv).wait_send()

    if n_rows > 1:

        @pl.when(is_first)
        def _():
            all_of(0, n_rows - 1, zero_send, ahead_recv).wait_send()

    widen.wait()
    fold_out[...] = fold[...]
    if n_rows > 1:
        all_of(1, n_rows - 1, all_send, all_recv).wait()

        @pl.when(is_first)
        def _():
            all_of(0, n_rows - 1, zero_send, ahead_recv).wait_recv()

    @pl.when(has_before)
    def _():
        all_of(0, n_rows, ahead_send, ahead_recv).wait_recv()

    block_out[...] = gathered[...]


def project(block, fold, shift, gram, out, held, sems):
    pdim, width = fold.shape
    frames, n_rows, tokens, _ = block.shape
    total = n_rows * tokens
    cuts = [0, 16, 48, 96] + list(range(144, total, 48)) + [total]
    copies = []
    for f in range(frames):
        patches = block[f].reshape(total, LANES)[:, :pdim]
        for n, (low, high) in enumerate(zip(cuts, cuts[1:])):
            own = patches[low:high]
            moved = dot(own, gram[0]) + dot(own, gram[1]) + dot(own, gram[2])
            spread = jnp.maximum(jnp.sum(moved * own.astype(F32), axis=-1, keepdims=True), 0.0)
            here = pl.ds(f * total + low, high - low)
            held[here] = dot(own, fold[...]) * lax.rsqrt(spread + EPS) + shift[...]
            copy = pltpu.make_async_copy(held.at[here], out.at[here], sems.at[len(copies)])
            copy.start()
            copies.append(copy)
    for copy in copies:
        copy.wait()


def per_device(
    n_groups, n_tm, n_rows,
    features, spatial_weight, temporal_weight, head_weight, embed_weight, ada_scale, ada_shift, qkv_weight,
):
    frames, rows, columns, channels = features.shape
    depth, width = qkv_weight.shape
    pdim, wide_all = embed_weight.shape
    latent = head_weight.shape[1]
    split = n_groups == 2
    depth = depth // 2 if split else depth
    aligned = depth % LANES == 0
    quads = (2 if split else 1) * (2 if n_tm >= 4 else 1)
    later = max(n_tm.bit_length() - 3, 0)
    block_rows = pdim // (2 * quads)
    fold_shape = (2, quads, block_rows, width)
    part = embed_weight
    scale, shift = (v.reshape(wide_all // LANES, LANES) for v in (ada_scale, ada_shift))
    if not aligned:
        scale, shift = ada_scale[None], ada_shift[None]
        start = lax.axis_index("tm") * qkv_weight.shape[0]
        if split:
            start = start + lax.axis_index("groups") * depth
        scale, shift, part = (lax.dynamic_slice_in_dim(v, start, depth, axis=1) for v in (scale, shift, part))
    hbm = pl.BlockSpec(memory_space=pl.ANY)
    vmem = pl.BlockSpec(memory_space=pltpu.VMEM)
    tokens = columns // PATCH
    dma = pltpu.SemaphoreType.DMA
    block, fold, shift_row, gram = pl.pallas_call(
        functools.partial(encode, n_tm, n_rows, split, aligned),
        out_shape=(
            pltpu.VMEM((frames, n_rows, tokens, LANES), BF16),
            pltpu.VMEM(fold_shape, BF16),
            pltpu.VMEM((1, width), F32),
            pltpu.VMEM((3, pdim, pdim), BF16),
        ),
        in_specs=[hbm] * 9,
        out_specs=(vmem, vmem, vmem, vmem),
        scratch_shapes=[
            pltpu.VMEM(features.shape, BF16),
            pltpu.VMEM((frames, 2, columns, channels), BF16),
            pltpu.VMEM((frames, columns, (rows + 2) * 3 * channels), BF16),
            pltpu.VMEM((9 * channels, channels), BF16),
            pltpu.VMEM((3, channels, channels), BF16),
            pltpu.VMEM((latent, channels), BF16),
            pltpu.VMEM((pdim, wide_all), BF16),
            pltpu.VMEM((pdim, depth), BF16),
            pltpu.VMEM(scale.shape, BF16),
            pltpu.VMEM(shift.shape, BF16),
            pltpu.VMEM((2, wide_all // LANES, LANES), F32),
            pltpu.VMEM((2 * pdim, wide_all), BF16),
            pltpu.VMEM((depth, width), BF16),
            pltpu.VMEM((frames, rows * columns, channels), BF16),
            pltpu.VMEM((frames, rows * columns, channels), BF16),
            pltpu.VMEM((rows * columns, channels), BF16),
            pltpu.VMEM((frames, rows * columns, channels), F32),
            pltpu.VMEM((columns, LANES), F32),
            pltpu.VMEM((tokens, LANES), BF16),
            pltpu.VMEM(fold_shape, BF16),
            pltpu.VMEM(fold_shape[1:], BF16),
            pltpu.VMEM(fold_shape, F32),
            pltpu.VMEM(fold_shape[1:], BF16),
            pltpu.VMEM(fold_shape[1:], BF16),
            pltpu.VMEM((max(2 * later, 1), block_rows, width), BF16),
            pltpu.VMEM(fold_shape, BF16),
            pltpu.VMEM((2 + later, 1, width), F32),
            pltpu.VMEM((quads + later, 1, width), F32),
            pltpu.VMEM((frames, n_rows, tokens, LANES), BF16),
            pltpu.VMEM((PATCH, channels, LANES), BF16),
            dma((9 if aligned else 10,)),
            dma((2,)), dma((frames, 2)),
            dma((2,)), dma((2,)),
            dma((1,)), dma((1,)), dma((1,)), dma((1,)), dma((1,)),
            dma((4 + later,)), dma((4 + later,)),
            dma((2 + later,)), dma((2 + later,)),
            pltpu.SemaphoreType.REGULAR((max(n_rows - 1, 1),)),
            pltpu.SemaphoreType.REGULAR((1,)),
        ],
        compiler_params=pltpu.CompilerParams(
            collective_id=0, has_side_effects=True, vmem_limit_bytes=56 * 2**20
        ),
        name="encode",
    )(
        features,
        spatial_weight.reshape(9 * channels, channels),
        temporal_weight,
        head_weight.T,
        embed_weight,
        part,
        scale,
        shift,
        qkv_weight,
    )
    count = frames * n_rows * tokens
    return pl.pallas_call(
        project,
        out_shape=jax.ShapeDtypeStruct((count, width), F32),
        in_specs=[vmem] * 4,
        out_specs=hbm,
        scratch_shapes=[pltpu.VMEM((count, width), F32), dma((count // 48 + 4 * frames,))],
        compiler_params=pltpu.CompilerParams(vmem_limit_bytes=32 * 2**20),
        name="project",
    )(block, fold.reshape(pdim, width), shift_row, gram)


def solution(mesh):
    return jax.shard_map(
        functools.partial(per_device, mesh.shape["groups"], mesh.shape["tm"], mesh.shape["rows"]),
        mesh=mesh,
        in_specs=(
            P(("groups", "tm"), "rows", None, None),
            P(),
            P(),
            P(),
            P(),
            P(),
            P(),
            P("tm", "rows"),
        ),
        out_specs=P(("groups", "tm"), "rows"),
        check_vma=False,
    )
```
